32 devices in a mesh: dp: 8 (over z, x), shard: 4 (over y, core).
Axes of the slice: x: 2, y: 2, z: 4, core: 2. Of those that a mesh axis runs over, the one named last changes fastest.
Arguments:
- tokens: bfloat16 [128, 3584], P('dp', 'shard'), may hold values from -6 to 6
- targets: bfloat16 [128, 3584], P('dp', 'shard'), may hold values from -6 to 6
- task_of_token: int32 [128], P('dp'), may hold values from 0 to 15, never falling along the last dimension, each value on 1 to 16 neighbouring positions
- up_weight: bfloat16 [18944, 3584], P('dp', 'shard'), may hold values from -0.09375 to 0.09375
- down_weight: bfloat16 [18944, 3584], P('dp', 'shard'), may hold values from -0.046875 to 0.046875
- outer_up: bfloat16 [18944, 3584], P('dp', 'shard'), may hold values from -6 to 6
- outer_down: bfloat16 [18944, 3584], P('dp', 'shard'), may hold values from -6 to 6
Outputs:
- meta_up: float32 [18944, 3584], P('dp', 'shard')
- meta_down: float32 [18944, 3584], P('dp', 'shard')
The draws below stay inside these ranges and needn't reach their ends.
Inputs may be any that keep to these rules, and one draw needn't show every extreme that they name: `task_of_token`: task numbers never fall along the tokens; every task has 1 to 16 tokens, and some task has exactly 16.
All inputs are finite; a program needn't handle non-finite values.
Results may differ from the reference program's by a relative error of at most 0.001.
Values may be sent and summed in bfloat16 or wider, within the bound.
A program may use at most 64 MiB of HBM per device.

```python
import math
import jax
import jax.numpy as jnp
import numpy as np
from jax import lax

D = 3584
FF = 18944
TASKS = 16
ITERS = 2
TOKENS = 128
MOST = 16


def level_of(own_key, extent, shards, smallest, high):
    gain = 1.0
    for position, parts in shards:
        draws = jax.random.uniform(jax.random.fold_in(jax.random.fold_in(own_key, 6), position), (parts,), jnp.float32, smallest / len(shards), high / len(shards))
        gain = gain * jnp.repeat(jnp.exp(draws), extent[position] // parts).reshape((-1,) + (1,) * (len(extent) - 1 - position))
    return gain


def profile(number_of, total, reach, skew):
    portions = [(1 << 20) // math.isqrt(rank ** skew) + 1 for rank in range(2, number_of + 1)]
    spare, holding = total - reach - (number_of - 1), [1] * (number_of - 1)
    while spare > 0:
        candidates = [i for i in range(number_of - 1) if holding[i] < reach]
        whole, left = sum([portions[i] for i in candidates]), spare
        for i in candidates:
            extra = min(reach - holding[i], max(1, left * portions[i] // whole), spare)
            holding[i] = holding[i] + extra
            spare = spare - extra
    return np.array([reach] + holding)


def ragged(key, count, total, most, skew):
    if count == 2:
        one = jax.random.randint(key, (), max(1, total - most), min(most, total - 1) + 1)
        return jnp.stack([one, total - one])
    lengths = jnp.asarray(profile(count, total, most, skew), jnp.int32)
    twos = (count - 1) // 2
    giver, sink = lengths[1:1 + 2 * twos:2], lengths[2:2 + 2 * twos:2]
    margin = jnp.minimum(giver - 1, most - sink)
    shifted = jax.random.randint(jax.random.fold_in(key, 1), (twos,), 0, 1 << 20) % (margin + 1)
    lengths = lengths.at[1:1 + 2 * twos:2].set(giver - shifted).at[2:2 + 2 * twos:2].set(sink + shifted)
    return lengths[jax.random.permutation(jax.random.fold_in(key, 2), count)]


def gaussian(rng, shape, scale, most, shards=(), held_as=jnp.bfloat16):
    array = scale * jax.random.normal(rng, shape, jnp.float32)
    if shards:
        array = array * level_of(rng, shape, shards, -0.22, 0.18)
    return jnp.clip(array, -most, most).astype(held_as)


def setup_inputs(seed: int = 0) -> dict:
    splits = jax.random.split(jax.random.key(seed), 8)
    return {
        "tokens": gaussian(splits[0], (TOKENS, D), 1.0, 6.0, ((0, 8), (1, 4))),
        "targets": gaussian(splits[1], (TOKENS, D), 1.0, 6.0, ((0, 8), (1, 4))),
        "task_of_token": jnp.searchsorted(jnp.cumsum(ragged(splits[2], TASKS, TOKENS, MOST, 0)), jnp.arange(TOKENS), side="right").astype(jnp.int32),
        "up_weight": gaussian(splits[3], (FF, D), D ** -0.5, 0.09375, ((0, 8), (1, 4))),
        "down_weight": gaussian(splits[4], (FF, D), FF ** -0.5, 0.046875, ((0, 8), (1, 4))),
        "outer_up": gaussian(splits[5], (FF, D), 1.0, 6.0, ((0, 8), (1, 4))),
        "outer_down": gaussian(splits[6], (FF, D), 1.0, 6.0, ((0, 8), (1, 4))),
    }


def sigmoid_parts(linear_part):
    argument = linear_part.astype(jnp.float32)
    logistic = jax.nn.sigmoid(argument)
    derivative = logistic * (1.0 + argument * (1.0 - logistic))
    second_order = logistic * (1.0 - logistic) * (2.0 + argument * (1.0 - 2.0 * logistic))
    return argument * logistic, derivative, second_order


def contract_last(left_side, right_side):
    return lax.dot_general(left_side, right_side, (((1,), (1,)), ((), ())), preferred_element_type=jnp.float32)


def contract_first(left_side, right_side):
    return lax.dot_general(left_side, right_side, (((0,), (0,)), ((), ())), preferred_element_type=jnp.float32)


def stored(values):
    return lax.optimization_barrier(values.astype(jnp.bfloat16))


def reference(tokens, targets, task_of_token, up_weight, down_weight, outer_up, outer_down):
    task_index = jnp.arange(TASKS, dtype=jnp.int32)
    members = (task_of_token[:, None] == task_index[None, :]).astype(jnp.float32)
    task_counts = jnp.sum(members, axis=0)
    inverse = 1.0 / (TASKS * task_counts)
    weight = jnp.sum(members * inverse[None, :], axis=1)
    linear_part = stored(contract_last(tokens, up_weight))
    activation, derivative, second_order = sigmoid_parts(linear_part)
    hidden = activation.astype(jnp.bfloat16)
    output_rows = jnp.dot(hidden, down_weight, preferred_element_type=jnp.float32)
    errors = (weight[:, None] * (output_rows - targets.astype(jnp.float32))).astype(jnp.bfloat16)
    backward = stored(contract_last(errors, down_weight)).astype(jnp.float32)

    def operator(vector_up, vector_down):
        direction_up = vector_up.astype(jnp.bfloat16)
        direction_down = vector_down.astype(jnp.bfloat16)
        tangent_linear = stored(contract_last(tokens, direction_up)).astype(jnp.float32)
        tangent_hidden = (derivative * tangent_linear).astype(jnp.bfloat16)
        tangent_output = jnp.dot(tangent_hidden, down_weight, preferred_element_type=jnp.float32)
        tangent_output = tangent_output + jnp.dot(hidden, direction_down, preferred_element_type=jnp.float32)
        tangent_errors = (weight[:, None] * tangent_output).astype(jnp.bfloat16)
        tangent_backward = stored(contract_last(tangent_errors, down_weight) + contract_last(errors, direction_down))
        tangent_gate = (derivative * tangent_backward.astype(jnp.float32) + second_order * backward * tangent_linear).astype(jnp.bfloat16)
        hessian_up = contract_first(tangent_gate, tokens)
        hessian_down = contract_first(tangent_hidden, errors) + contract_first(hidden, tangent_errors)
        return vector_up + hessian_up, vector_down + hessian_down

    residual_up = outer_up.astype(jnp.float32)
    residual_down = outer_down.astype(jnp.float32)
    solution_up = jnp.zeros_like(residual_up)
    solution_down = jnp.zeros_like(residual_down)
    search_up, search_down = residual_up, residual_down
    norm_now = jnp.sum(residual_up * residual_up) + jnp.sum(residual_down * residual_down)
    for iteration in range(ITERS):
        image_up, image_down = operator(search_up, search_down)
        step_size = norm_now / (jnp.sum(search_up * image_up) + jnp.sum(search_down * image_down))
        solution_up = solution_up + step_size * search_up
        solution_down = solution_down + step_size * search_down
        residual_up = residual_up - step_size * image_up
        residual_down = residual_down - step_size * image_down
        norm_next = jnp.sum(residual_up * residual_up) + jnp.sum(residual_down * residual_down)
        ratio_next = norm_next / norm_now
        search_up = residual_up + ratio_next * search_up
        search_down = residual_down + ratio_next * search_down
        norm_now = norm_next
    return solution_up, solution_down
```

```python
import functools
import types

import jax
import jax.numpy as jnp
from jax import lax
from jax.experimental import pallas as pl
from jax.experimental.pallas import tpu as pltpu
from jax.sharding import PartitionSpec as P

TASKS = 16
STEPS = 4
BF = jnp.bfloat16
F32 = jnp.float32
MESH = pl.DeviceIdType.MESH
VMEM_LIMIT = 60 * 2**20


def sigmoid_parts(linear_part):
    argument = linear_part.astype(F32)
    logistic = jax.nn.sigmoid(argument)
    derivative = logistic * (1.0 + argument * (1.0 - logistic))
    second_order = logistic * (1.0 - logistic) * (2.0 + argument * (1.0 - 2.0 * logistic))
    return (argument * logistic, derivative, second_order)


def contract_last(left_side, right_side):
    return lax.dot_general(
        left_side, right_side, (((1,), (1,)), ((), ())), preferred_element_type=F32
    )


def contract_first(left_side, right_side):
    return lax.dot_general(
        left_side, right_side, (((0,), (0,)), ((), ())), preferred_element_type=F32
    )


def product(left_side, right_side):
    return jnp.dot(left_side, right_side, preferred_element_type=F32)


def remote(src, dst, send_sem, recv_sem, where):
    return pltpu.make_async_remote_copy(
        src_ref=src,
        dst_ref=dst,
        send_sem=send_sem,
        recv_sem=recv_sem,
        device_id=where,
        device_id_type=MESH,
    )


def summed(term):
    return jnp.sum(jnp.sum(term, axis=1, keepdims=True), axis=0, keepdims=True)


def folded(term):
    return jnp.sum(term.reshape(term.shape[0] // 8, 8, term.shape[1]), axis=0)


def span(start, size, unit):
    return pl.ds(pl.multiple_of(start, unit), size)


def fused_kernel(n, m, hid, names, *refs):
    r = types.SimpleNamespace(**dict(zip(names, refs)))
    rows, width = r.tokens.shape
    count, half, nz = n * rows, n * rows // 2, n // 2
    total = r.w.shape[1]
    hp = total // 2
    h = hp // STEPS
    bits = m.bit_length() - 1
    me = lax.axis_index("dp")
    xx, zz = lax.rem(me, 2), me // 2
    shard = lax.axis_index("shard")
    low = lax.rem(shard, 2)
    mine, other = low * hp, (1 - low) * hp
    partner = {"dp": 2 * zz + 1 - xx}
    column = [{"dp": 2 * lax.rem(zz + k, nz) + xx} for k in range(1, nz)]
    dp_places = [{"dp": lax.rem(me + k, n)} for k in range(1, n)]
    shard_places = [{"shard": lax.rem(shard + k, m)} for k in range(1, m)]

    def flip(bit):
        step = 1 << bit
        return {"shard": shard + step - 2 * step * lax.rem(shard // step, 2)}

    loads = [
        pltpu.make_async_copy(src, r.w.at[i, pl.ds(0, hid)], r.load_sem.at[i])
        for i, src in enumerate((r.up, r.outer_up, r.down, r.outer_down))
    ]
    for load in loads:
        load.start()

    lane = lax.broadcasted_iota(jnp.int32, (8, 128), 1)
    line = lax.broadcasted_iota(jnp.int32, (rows, 128), 0)
    own_row = jnp.full((8, 128), -1.0, F32)
    own_col = jnp.zeros((rows, 128), F32)
    for i in range(rows):
        number = r.task[i].astype(F32)
        own_row = jnp.where(lane == i, number, own_row)
        own_col = jnp.where(line == i, number, own_col)
    r.task_own[...] = own_row
    place = xx * nz + zz
    block = span(place * rows, rows, rows)
    r.xx[block, :] = r.tokens[...]
    if total > hid:
        r.w[:, pl.ds(hid, total - hid), :] = jnp.zeros((4, total - hid, width), BF)
    r.acc[...] = jnp.zeros(r.acc.shape, F32)

    barrier = pltpu.get_barrier_semaphore()
    for where in dp_places + shard_places:
        pl.semaphore_signal(barrier, inc=1, device_id=where, device_id_type=MESH)
    pl.semaphore_wait(barrier, n + m - 2)

    def spread(s, src, dst, offset):
        to = span(offset + place * rows, rows, rows)
        out = [
            remote(src, dst.at[to, :], r.sp_zs.at[s, k], r.sp_zr.at[s, k], column[k])
            for k in range(nz - 1)
        ]
        out.append(remote(src, dst.at[to, :], r.sp_xs.at[s, 0], r.sp_xr.at[s, 0], partner))
        for copy in out:
            copy.start()
        return out

    def forward(s, dst, offset, out):
        for k in range(1, nz):
            out[k - 1].wait_recv()
            at = span(offset + (xx * nz + lax.rem(zz + nz - k, nz)) * rows, rows, rows)
            copy = remote(
                dst.at[at, :], dst.at[at, :], r.sp_xs.at[s, k], r.sp_xr.at[s, k], partner
            )
            copy.start()
            out.append(copy)

    def arrived(out):
        for copy in out[nz - 1 :]:
            copy.wait_recv()

    token_copies = spread(0, r.tokens, r.xx, 0)
    task_copies = [
        remote(r.task_own, r.task_slots.at[k], r.task_s.at[k], r.task_r.at[k], dp_places[k])
        for k in range(n - 1)
    ]
    for copy in task_copies:
        copy.start()
    forward(0, r.xx, 0, token_copies)
    arrived(token_copies)
    for load in loads:
        load.wait()
    tokens = r.xx

    def first_hop(s, i):
        at = span(i * h, h, 16)
        return remote(
            r.part.at[s, at, :], r.got.at[s, at, :], r.ex_s.at[s, 0, i], r.ex_r.at[s, 0, i], flip(0)
        )

    def wire_hop(s, bit, i):
        at = span(i * h, h, 16)
        return remote(
            r.sent.at[s, bit - 1, at, :],
            r.wire.at[s, bit - 1, at, :],
            r.ex_s.at[s, bit, i],
            r.ex_r.at[s, bit, i],
            flip(bit),
        )

    full = [r.full.at[0], r.full.at[1], r.gate]

    def last_hop(s, i):
        at = span(mine + i * h, h, 16)
        return remote(
            full[s].at[at, :], full[s].at[at, :], r.ex_s.at[s, bits, i], r.ex_r.at[s, bits, i], flip(0)
        )

    def send_chunks(s, make):
        def own_half(i):
            at = span(i * h, h, 16)
            first_hop(s, i).wait_recv()
            value = (r.keep[at, :] + r.got[s, at, :].astype(F32)).astype(BF)
            if bits > 1:
                r.sent[s, 0, at, :] = value
                wire_hop(s, 1, i).start()
            else:
                r.part_own[at, :] = value

        def step(i, _):
            at = span(i * h, h, 16)
            r.part[s, at, :] = make(other + i * h).astype(BF)
            first_hop(s, i).start()
            r.keep[at, :] = make(mine + i * h)

            @pl.when(i > 0)
            def _():
                own_half(i - 1)

            return 0

        lax.fori_loop(0, STEPS, step, 0)
        own_half(STEPS - 1)

    def take_chunks(s, use, begin, end):
        def step(i, _):
            at = span(i * h, h, 16)
            for bit in range(1, bits):
                wire_hop(s, bit, i).wait_recv()
                value = r.sent[s, bit - 1, at, :].astype(F32) + r.wire[s, bit - 1, at, :].astype(F32)
                value = value.astype(BF)
                if bit + 1 < bits:
                    r.sent[s, bit, at, :] = value
                    wire_hop(s, bit + 1, i).start()
            full[s][span(mine + i * h, h, 16), :] = value
            last_hop(s, i).start()
            use(mine + i * h)
            last_hop(s, i).wait_recv()
            use(other + i * h)
            return 0

        lax.fori_loop(begin, end, step, 0)

    def linear_rows(kind):
        def make(row):
            return contract_last(r.w[kind, span(row, h, 16), :], tokens[...])

        return make

    def hidden_rows(row):
        at = span(row, h, 16)
        activation, derivative, second_order = sigmoid_parts(r.full[0, at, :])
        hidden = activation.astype(BF)
        r.both[at, count:] = hidden
        r.derivative[at, :] = derivative
        r.second[at, :] = second_order
        r.acc[0] += contract_first(hidden, r.w[2, at, :])
        r.acc[1] += contract_first(hidden, r.w[3, at, :])

    def tangent_rows(row):
        at = span(row, h, 16)
        tangent = (r.derivative[at, :] * r.full[1, at, :].astype(F32)).astype(BF)
        r.both[at, :count] = tangent
        r.acc[1] += contract_first(tangent, r.w[2, at, :])

    own_half_rows = span(xx * half, half, half)

    def reduce_start(s):
        r.half_out[s] = r.acc[s, span((1 - xx) * half, half, half), :].astype(BF)
        copy = remote(r.half_out.at[s], r.half_in.at[s], r.rx_s.at[s], r.rx_r.at[s], partner)
        copy.start()
        return [copy]

    def reduce_middle(s, out):
        out[0].wait_recv()
        value = r.acc[s, own_half_rows, :] + r.half_in[s].astype(F32)
        r.acc[s, own_half_rows, :] = value
        r.column_out[s] = value.astype(BF)
        for k in range(1, nz):
            copy = remote(
                r.column_out.at[s, span(lax.rem(zz + k, nz) * rows, rows, rows), :],
                r.column_in.at[s, k - 1],
                r.rz_s.at[s, k - 1],
                r.rz_r.at[s, k - 1],
                column[k - 1],
            )
            copy.start()
            out.append(copy)

    def reduce_end(s, out):
        value = r.acc[s, block, :]
        for k in range(1, nz):
            out[k].wait_recv()
            value = value + r.column_in[s, k - 1].astype(F32)
        return value

    k_mine, k_other = span(low * half, half, half), span((1 - low) * half, half, half)

    def gram_copy(j):
        if j == 0:
            src, dst = r.token_gram.at[k_other, :], r.gram_got
        elif j < bits:
            src, dst = r.gram_sent.at[j - 1], r.gram_wire.at[j - 1]
        else:
            src, dst = r.gram_full.at[k_mine, :], r.gram_full.at[k_mine, :]
        return remote(src, dst, r.gram_s.at[j], r.gram_r.at[j], flip(0 if j == bits else j))

    def gram_step(j):
        if j == 0:
            r.token_gram[...] = contract_last(tokens[...], tokens[...])
            gram_copy(0).start()
            return
        gram_copy(j - 1).wait_recv()
        if j == 1:
            value = r.token_gram[k_mine, :] + r.gram_got[...]
        elif j <= bits:
            value = r.gram_sent[j - 2] + r.gram_wire[j - 2]
        if j < bits:
            r.gram_sent[j - 1] = value
        elif j == bits:
            r.gram_full[k_mine, :] = value
        if j <= bits:
            gram_copy(j).start()
            return
        high = r.gram_full[...].astype(BF)
        r.gram_parts[0] = high
        r.gram_parts[1] = (r.gram_full[...] - high.astype(F32)).astype(BF)

    send_chunks(0, linear_rows(0))
    send_chunks(1, linear_rows(1))
    gram_step(0)
    take_chunks(0, hidden_rows, 0, STEPS)
    y_copies = reduce_start(0)
    gram_step(1)
    take_chunks(1, tangent_rows, 0, STEPS // 2)
    reduce_middle(0, y_copies)
    take_chunks(1, tangent_rows, STEPS // 2, STEPS)
    z_copies = reduce_start(1)
    for j in range(2, bits + 1):
        gram_step(j)

    same = jnp.where(own_row[0:1, :] == own_col, 1.0, 0.0)
    for k, copy in enumerate(task_copies):
        copy.wait_recv()
        same = same + jnp.where(r.task_slots[k, 0:1, :] == own_col, 1.0, 0.0)
    weight = 1.0 / (TASKS * jnp.sum(same, axis=1, keepdims=True))

    value = reduce_end(0, y_copies)
    r.fresh[0] = (weight * (value - r.targets[...].astype(F32))).astype(BF)
    r.ee[block, :] = r.fresh[0]
    e_copies = spread(1, r.fresh.at[0], r.ee, 0)
    reduce_middle(1, z_copies)

    def gram_rows(kind):
        at = span(kind * h, h, 16)
        r.both_gram[...] += contract_first(r.both[at, :], r.both[at, :])

    r.both_gram[...] = jnp.zeros(r.both_gram.shape, F32)
    lax.fori_loop(0, 2 * STEPS, lambda i, _: (gram_rows(i), 0)[1], 0)
    forward(1, r.ee, 0, e_copies)
    value = reduce_end(1, z_copies)
    first = summed(weight * (value * value))
    r.fresh[1] = (weight * value).astype(BF)
    r.ee[span(count + place * rows, rows, rows), :] = r.fresh[1]
    t_copies = spread(2, r.fresh.at[1], r.ee, count)
    arrived(e_copies)

    def error_rows(i, kept):
        at = span(i * h, h, 16)
        errors = r.ee[pl.ds(0, count), :]
        back = contract_last(r.w[2, at, :], errors)
        crossing = contract_last(r.w[3, at, :], errors)
        tangent = r.full[1, at, :].astype(F32)
        curved = r.second[at, :] * back
        r.curved[at, :] = curved
        r.gate_base[at, :] = r.derivative[at, :] * crossing + curved * tangent
        term = 2.0 * r.both[at, :count].astype(F32) * crossing + curved * tangent * tangent
        return kept + folded(term)

    kept = lax.fori_loop(0, 2 * STEPS, error_rows, jnp.zeros((8, count), F32))
    first = first * jnp.ones((1, 128), F32)
    first_part = summed(kept)
    gram_step(bits + 1)

    def norm_rows(i, kept):
        at = span(i * 16, 16, 16)
        one, two = r.w[1, at, :].astype(F32), r.w[3, at, :].astype(F32)
        return kept + one * one + two * two

    norm = summed(lax.fori_loop(0, total // 16, norm_rows, jnp.zeros((16, width), F32)))
    forward(2, r.ee, count, t_copies)
    arrived(t_copies)

    def gate_make(row):
        at = span(row, h, 16)
        back = contract_last(r.w[2, at, :], r.ee[pl.ds(count, count), :])
        return r.gate_base[at, :] + r.derivative[at, :] * back

    r.kept[...] = jnp.zeros(r.kept.shape, F32)
    r.gate_gram[...] = jnp.zeros(r.gate_gram.shape, F32)
    r.carry_gram[...] = jnp.zeros(r.carry_gram.shape, F32)

    def gate_rows(row):
        at = span(row, h, 16)
        gate = r.gate[at, :]
        lowered = product(gate, r.gram_parts[0]) + product(gate, r.gram_parts[1])
        carried = (r.derivative[at, :] * lowered).astype(BF)
        r.acc[2] += contract_first(carried, r.w[2, at, :])
        r.gate_gram[...] += contract_first(gate, gate)
        r.carry_gram[...] += contract_first(carried, r.both[at, :])
        r.kept[...] += folded(r.curved[at, :] * lowered * lowered)

    send_chunks(2, gate_make)
    take_chunks(2, gate_rows, 0, STEPS)
    head, tail = pl.ds(0, count), pl.ds(count, count)
    r.acc[2] += product(r.both_gram[tail, :].astype(BF), r.ee[...])
    w_copies = reduce_start(2)

    gram = contract_last(r.ee[...], r.ee[...])
    h_t = summed(r.both_gram[tail, head] * gram[count:, :count])
    change = summed(r.gate_gram[...] * r.token_gram[...]) + 2.0 * h_t
    change = change + summed(r.both_gram[head, head] * gram[:count, :count])
    change = change + summed(r.both_gram[tail, tail] * gram[count:, count:])
    carry = summed(r.carry_gram[:, head] * gram[:count, :count])
    carry = carry + summed(r.carry_gram[:, tail] * gram[:count, count:])
    final = summed(r.kept[...]) + 2.0 * carry

    reduce_middle(2, w_copies)
    value = reduce_end(2, w_copies)
    final = final + summed(weight * (value * value))
    index = lax.broadcasted_iota(jnp.int32, (8, 128), 0)
    value = jnp.zeros((8, 128), F32)
    for at, number in enumerate((norm, first + first_part, change, final)):
        value = value + jnp.where(index == at, number, 0.0)
    r.own[0] = value
    dp_copies = [
        remote(r.own.at[0], r.dp_slots.at[k], r.dp_s.at[k], r.dp_r.at[k], dp_places[k])
        for k in range(n - 1)
    ]
    for copy in dp_copies:
        copy.start()
    for k, copy in enumerate(dp_copies):
        copy.wait_recv()
        value = value + r.dp_slots[k]
    r.own[1] = value
    shard_copies = [
        remote(r.own.at[1], r.shard_slots.at[k], r.sh_s.at[k], r.sh_r.at[k], shard_places[k])
        for k in range(m - 1)
    ]
    for copy in shard_copies:
        copy.start()
    for k, copy in enumerate(shard_copies):
        copy.wait_recv()
        value = value + r.shard_slots[k]
    r.own[2] = value
    norm, first, change, final = (r.own[2, i : i + 1, :] for i in range(4))
    step = norm / (norm + first)
    keep = first / (norm + first)
    norm_next = keep * keep * norm - 2.0 * keep * step * first + step * step * change
    ratio = norm_next / norm
    curvature = (
        norm_next
        + keep * keep * first
        - 2.0 * keep * step * change
        + step * step * final
        - ratio * norm_next / step
    )
    step_next = norm_next / curvature
    r.sums[0:1, :] = step + step_next * (ratio + keep)
    r.sums[1:2, :] = -step_next * step

    def sends_done(i, _):
        for s in range(3):
            first_hop(s, i).wait_send()
            for bit in range(1, bits):
                wire_hop(s, bit, i).wait_send()
            last_hop(s, i).wait_send()
        return 0

    lax.fori_loop(0, STEPS, sends_done, 0)
    for j in range(bits + 1):
        gram_copy(j).wait_send()
    for copy in token_copies + e_copies + t_copies + y_copies + z_copies + w_copies:
        copy.wait_send()
    for copy in task_copies + dp_copies + shard_copies:
        copy.wait_send()


def fused(n, m, tokens, targets, task, up, outer_up, down, outer_down):
    hid, width = up.shape
    rows = tokens.shape[0]
    count, half, nz = n * rows, n * rows // 2, n // 2
    bits = m.bit_length() - 1
    hp = -(-hid // (2 * 16 * STEPS)) * 16 * STEPS
    total = 2 * hp
    vm, dma = pltpu.VMEM, pltpu.SemaphoreType.DMA
    links = max(bits - 1, 1)
    outs = {
        "gate": ((total, count), BF),
        "both": ((total, 2 * count), BF),
        "xx": ((count, width), BF),
        "ee": ((2 * count, width), BF),
        "sums": ((8, 128), F32),
    }
    scratch = {
        "w": vm((4, total, width), BF),
        "part": vm((3, hp, count), BF),
        "keep": vm((hp, count), F32),
        "got": vm((3, hp, count), BF),
        "sent": vm((3, links, hp, count), BF),
        "wire": vm((3, links, hp, count), BF),
        "full": vm((2, total, count), BF),
        "derivative": vm((total, count), F32),
        "second": vm((total, count), F32),
        "curved": vm((total, count), F32),
        "gate_base": vm((total, count), F32),
        "acc": vm((3, count, width), F32),
        "half_out": vm((3, half, width), BF),
        "half_in": vm((3, half, width), BF),
        "column_out": vm((3, half, width), BF),
        "column_in": vm((3, nz - 1, rows, width), BF),
        "fresh": vm((2, rows, width), BF),
        "token_gram": vm((count, count), F32),
        "gram_got": vm((half, count), F32),
        "gram_sent": vm((links, half, count), F32),
        "gram_wire": vm((links, half, count), F32),
        "gram_full": vm((count, count), F32),
        "gram_parts": vm((2, count, count), BF),
        "both_gram": vm((2 * count, 2 * count), F32),
        "gate_gram": vm((count, count), F32),
        "carry_gram": vm((count, 2 * count), F32),
        "kept": vm((8, count), F32),
        "task_own": vm((8, 128), F32),
        "task_slots": vm((n - 1, 8, 128), F32),
        "own": vm((3, 8, 128), F32),
        "dp_slots": vm((n - 1, 8, 128), F32),
        "shard_slots": vm((m - 1, 8, 128), F32),
        "load_sem": dma((4,)),
        "task_s": dma((n - 1,)),
        "task_r": dma((n - 1,)),
        "sp_zs": dma((3, nz - 1)),
        "sp_zr": dma((3, nz - 1)),
        "sp_xs": dma((3, nz)),
        "sp_xr": dma((3, nz)),
        "ex_s": dma((3, bits + 1, STEPS)),
        "ex_r": dma((3, bits + 1, STEPS)),
        "rx_s": dma((3,)),
        "rx_r": dma((3,)),
        "rz_s": dma((3, nz - 1)),
        "rz_r": dma((3, nz - 1)),
        "gram_s": dma((bits + 1,)),
        "gram_r": dma((bits + 1,)),
        "dp_s": dma((n - 1,)),
        "dp_r": dma((n - 1,)),
        "sh_s": dma((m - 1,)),
        "sh_r": dma((m - 1,)),
    }
    inputs = ("task", "tokens", "targets", "up", "outer_up", "down", "outer_down")
    whole = pl.BlockSpec(memory_space=pltpu.VMEM)
    return pl.pallas_call(
        functools.partial(fused_kernel, n, m, hid, inputs + tuple(outs) + tuple(scratch)),
        out_shape=[jax.ShapeDtypeStruct(*o) for o in outs.values()],
        in_specs=[pl.BlockSpec(memory_space=pltpu.SMEM), whole, whole]
        + [pl.BlockSpec(memory_space=pl.ANY)] * 4,
        out_specs=[whole] * len(outs),
        scratch_shapes=list(scratch.values()),
        compiler_params=pltpu.CompilerParams(
            collective_id=0, has_side_effects=True, vmem_limit_bytes=VMEM_LIMIT
        ),
    )(task, tokens, targets, up, outer_up, down, outer_down)


def output_kernel(sums, gate, both, xx, ee, outer_up, outer_down, meta_up, meta_down):
    of_outer, of_change = sums[0:1, 0:1], sums[1:2, 0:1]
    meta_up[...] = of_outer * outer_up[...].astype(F32) + of_change * product(gate[...], xx[...])
    change = product(both[...], ee[...])
    meta_down[...] = of_outer * outer_down[...].astype(F32) + of_change * change


def outputs(gate, both, xx, ee, sums, outer_up, outer_down):
    hid, width = outer_up.shape
    tile = max(t for t in range(16, 601, 16) if hid % t == 0)

    def tiled(columns):
        return pl.BlockSpec((tile, columns), lambda i: (i, 0))

    def whole(array):
        return pl.BlockSpec(array.shape, lambda i: (0, 0))

    return pl.pallas_call(
        output_kernel,
        grid=(hid // tile,),
        out_shape=[jax.ShapeDtypeStruct((hid, width), F32)] * 2,
        in_specs=[
            whole(sums), tiled(gate.shape[1]), tiled(both.shape[1]), whole(xx), whole(ee),
            tiled(width), tiled(width),
        ],
        out_specs=[tiled(width)] * 2,
    )(sums, gate, both, xx, ee, outer_up, outer_down)


def body(n, m, tokens, targets, task_of_token, up_weight, down_weight, outer_up, outer_down):
    gate, both, xx, ee, sums = fused(
        n, m, tokens, targets, task_of_token, up_weight, outer_up, down_weight, outer_down
    )
    return tuple(outputs(gate, both, xx, ee, sums, outer_up, outer_down))


def solution(mesh):
    placed = tuple(P("dp") if i == 2 else P("dp", "shard") for i in range(7))
    return jax.shard_map(
        functools.partial(body, mesh.shape["dp"], mesh.shape["shard"]),
        mesh=mesh,
        in_specs=placed,
        out_specs=(P("dp", "shard"), P("dp", "shard")),
        check_vma=False,
    )
```

```python
import functools
import types

import jax
import jax.numpy as jnp
from jax import lax
from jax.experimental import pallas as pl
from jax.experimental.pallas import tpu as pltpu
from jax.sharding import PartitionSpec as P

TASKS = 16
STEPS = 4
BF = jnp.bfloat16
F32 = jnp.float32
MESH = pl.DeviceIdType.MESH
VMEM_LIMIT = 44 * 2**20
OUT_LIMIT = 24 * 2**20


def sigmoid_parts(linear_part):
    argument = linear_part.astype(F32)
    logistic = jax.nn.sigmoid(argument)
    derivative = logistic * (1.0 + argument * (1.0 - logistic))
    second_order = logistic * (1.0 - logistic) * (2.0 + argument * (1.0 - 2.0 * logistic))
    return (argument * logistic, derivative, second_order)


def contract_last(left_side, right_side):
    return lax.dot_general(
        left_side, right_side, (((1,), (1,)), ((), ())), preferred_element_type=F32
    )


def contract_first(left_side, right_side):
    return lax.dot_general(
        left_side, right_side, (((0,), (0,)), ((), ())), preferred_element_type=F32
    )


def product(left_side, right_side):
    return jnp.dot(left_side, right_side, preferred_element_type=F32)


def remote(src, dst, send_sem, recv_sem, where):
    return pltpu.make_async_remote_copy(
        src_ref=src,
        dst_ref=dst,
        send_sem=send_sem,
        recv_sem=recv_sem,
        device_id=where,
        device_id_type=MESH,
    )


def summed(term):
    return jnp.sum(jnp.sum(term, axis=1, keepdims=True), axis=0, keepdims=True)


def folded(term):
    return jnp.sum(term.reshape(term.shape[0] // 8, 8, term.shape[1]), axis=0)


def span(start, size, unit):
    return pl.ds(pl.multiple_of(start, unit), size)


def fused_kernel(n, m, hid, names, *refs):
    r = types.SimpleNamespace(**dict(zip(names, refs)))
    rows, width = r.tokens_in.shape
    count, half, nz = n * rows, n * rows // 2, n // 2
    total = r.both.shape[0]
    hp = total // 2
    h = hp // STEPS
    wide = 2 * h
    bits = m.bit_length() - 1
    me = lax.axis_index("dp")
    xx, zz = lax.rem(me, 2), me // 2
    shard = lax.axis_index("shard")
    low = lax.rem(shard, 2)
    partner = {"dp": 2 * zz + 1 - xx}

    def across(j):
        to = zz
        for bit in range(nz.bit_length() - 1):
            if j >> bit & 1:
                step = 1 << bit
                to = to + step - 2 * step * lax.rem(zz // step, 2)
        return to

    column = [{"dp": 2 * across(j) + xx} for j in range(nz)]
    far_first = range(nz - 1, 0, -1)
    dp_places = [{"dp": lax.rem(me + k, n)} for k in range(1, n)]
    shard_places = [{"shard": lax.rem(shard + k, m)} for k in range(1, m)]
    all_places = [
        {"dp": lax.rem(me + a, n), "shard": lax.rem(shard + b, m)}
        for a in range(n)
        for b in range(m)
        if a + b
    ]

    def flip(bit):
        step = 1 << bit
        return {"shard": shard + step - 2 * step * lax.rem(shard // step, 2)}

    barrier = pltpu.get_barrier_semaphore()
    for where in all_places:
        pl.semaphore_signal(barrier, inc=1, device_id=where, device_id_type=MESH)
    small = [
        pltpu.make_async_copy(src, dst, r.small_sem.at[i])
        for i, (src, dst) in enumerate(
            ((r.task_in, r.task), (r.tokens_in, r.tokens), (r.targets_in, r.targets))
        )
    ]
    small[1].start()
    small[0].start()

    def load(src, dst, step, index):
        size = min(wide, hid - step * wide)
        return pltpu.make_async_copy(
            src.at[pl.ds(step * wide, size)], dst.at[pl.ds(0, size)], r.load_sem.at[index, step]
        )

    loads = []
    for step in range(STEPS):
        if step * wide < hid:
            loads.append(load(r.up, r.ups.at[step, 0], step, 0))
            loads.append(load(r.outer_up, r.ups.at[step, 1], step, 1))
    for step in range(STEPS):
        if step * wide < hid:
            loads.append(load(r.down, r.low_down.at[pl.ds(step * wide, wide)], step, 2))
            loads.append(load(r.outer_down, r.outer_low.at[pl.ds(step * wide, wide)], step, 3))
    small[1].wait()
    small[0].wait()
    for copy in loads + small[2:]:
        copy.start()

    block = span(zz * rows, rows, rows)
    r.xx[block, :] = r.tokens[...]
    for step in range(STEPS):
        gap = min(wide, (step + 1) * wide - hid)
        if gap > 0:
            r.ups[step, :, pl.ds(wide - gap, gap), :] = jnp.zeros((2, gap, width), BF)
    if total > hid:
        r.low_down[pl.ds(hid, total - hid), :] = jnp.zeros((total - hid, width), BF)
        r.outer_low[pl.ds(hid, total - hid), :] = jnp.zeros((total - hid, width), BF)
    r.acc[...] = jnp.zeros(r.acc.shape, F32)

    pl.semaphore_wait(barrier, n * m - 1)

    def spread(s, src, dst, offset):
        near = span(offset + zz * rows, rows, rows)
        over = span(offset + half + zz * rows, rows, rows)
        out = [
            remote(src, dst.at[near, :], r.sp_zs.at[s, j - 1], r.sp_zr.at[s, j - 1], column[j])
            for j in far_first
        ]
        out.append(remote(src, dst.at[over, :], r.sp_xs.at[s, 0], r.sp_xr.at[s, 0], partner))
        for copy in out:
            copy.start()
        return out

    def forward(s, dst, offset, out):
        for j in range(1, nz):
            out[nz - 1 - j].wait_recv()
            at = span(offset + across(j) * rows, rows, rows)
            over = span(offset + half + across(j) * rows, rows, rows)
            copy = remote(
                dst.at[at, :], dst.at[over, :], r.sp_xs.at[s, j], r.sp_xr.at[s, j], partner
            )
            copy.start()
            out.append(copy)

    def arrived(out):
        for copy in out[nz - 1 :]:
            copy.wait_recv()

    token_copies = spread(0, r.tokens, r.xx, 0)

    lane = lax.broadcasted_iota(jnp.int32, (8, 128), 1)
    line = lax.broadcasted_iota(jnp.int32, (rows, 128), 0)
    own_row = jnp.full((8, 128), -1.0, F32)
    own_col = jnp.zeros((rows, 128), F32)
    for i in range(rows):
        number = r.task[i].astype(F32)
        own_row = jnp.where(lane == i, number, own_row)
        own_col = jnp.where(line == i, number, own_col)
    r.task_own[...] = own_row
    task_copies = [
        remote(r.task_own, r.task_slots.at[k], r.task_s.at[k], r.task_r.at[k], dp_places[k])
        for k in range(n - 1)
    ]
    for copy in task_copies:
        copy.start()
    forward(0, r.xx, 0, token_copies)
    arrived(token_copies)
    for copy in loads + small[2:]:
        copy.wait()
    tokens = r.xx

    def chunk(i):
        return span(i * wide, wide, 16)

    def own_part(i):
        return span(i * wide + low * h, h, 16)

    def strip(i):
        return span(i * h, h, 16)

    full = [r.full.at[0], r.full.at[1], r.gate]

    def first_hop(s, i):
        away = span(i * wide + (1 - low) * h, h, 16)
        return remote(
            r.part.at[s, away, :], r.got.at[s, strip(i), :], r.ex_s.at[s, 0, i], r.ex_r.at[s, 0, i], flip(0)
        )

    def wire_hop(s, bit, i):
        return remote(
            r.sent.at[s, bit - 1, strip(i), :],
            r.wire.at[s, bit - 1, strip(i), :],
            r.ex_s.at[s, bit, i],
            r.ex_r.at[s, bit, i],
            flip(bit),
        )

    def last_hop(s, i):
        at = own_part(i)
        return remote(
            full[s].at[at, :], full[s].at[at, :], r.ex_s.at[s, bits, i], r.ex_r.at[s, bits, i], flip(0)
        )

    def pair_sum(s, i):
        first_hop(s, i).wait_recv()
        value = r.part[s, own_part(i), :].astype(F32) + r.got[s, strip(i), :].astype(F32)
        r.sent[s, 0, strip(i), :] = value.astype(BF)
        wire_hop(s, 1, i).start()

    def take_chunks(s, use, begin, end):
        def step(i, _):
            for bit in range(1, bits):
                wire_hop(s, bit, i).wait_recv()
                value = r.sent[s, bit - 1, strip(i), :].astype(F32)
                value = (value + r.wire[s, bit - 1, strip(i), :].astype(F32)).astype(BF)
                if bit + 1 < bits:
                    r.sent[s, bit, strip(i), :] = value
                    wire_hop(s, bit + 1, i).start()
            full[s][own_part(i), :] = value
            last_hop(s, i).start()

            @pl.when(i > 0)
            def _():
                last_hop(s, i - 1).wait_recv()
                use(chunk(i - 1))

            return 0

        lax.fori_loop(begin, end, step, 0)
        if end == STEPS:
            use(own_part(STEPS - 1))
            last_hop(s, STEPS - 1).wait_recv()
            use(span((STEPS - 1) * wide + (1 - low) * h, h, 16))

    def linear_step(i, _):
        value = contract_last(r.ups[i].reshape(2 * wide, width), tokens[...])
        for s in range(2):
            r.part[s, chunk(i), :] = value[s * wide : (s + 1) * wide].astype(BF)
            first_hop(s, i).start()

        @pl.when(i > 0)
        def _():
            pair_sum(0, i - 1)

        return 0

    def hidden_rows(at):
        activation, derivative, second_order = sigmoid_parts(r.full[0, at, :])
        hidden = activation.astype(BF)
        r.both[at, count:] = hidden
        r.derivative[at, :] = derivative
        r.second[at, :] = second_order
        r.acc[0] += contract_first(hidden, r.low_down[at, :])
        r.acc[1] += contract_first(hidden, r.outer_low[at, :])

    def tangent_rows(at):
        tangent = (r.derivative[at, :] * r.full[1, at, :].astype(F32)).astype(BF)
        r.both[at, :count] = tangent
        r.acc[1] += contract_first(tangent, r.low_down[at, :])

    def half_place(j):
        return span(across(j) * rows, rows, rows)

    def half_copy(s, j):
        return remote(
            r.half_out.at[s, half_place(j), :], r.half_in.at[s, j], r.rx_s.at[s, j], r.rx_r.at[s, j], partner
        )

    def column_copy(s, j):
        return remote(
            r.column_out.at[s, j - 1], r.column_in.at[s, j - 1], r.rz_s.at[s, j - 1], r.rz_r.at[s, j - 1], column[j]
        )

    def reduce_start(s):
        r.half_out[s] = r.acc[s, pl.ds(half, half), :].astype(BF)
        for j in range(nz - 1, -1, -1):
            half_copy(s, j).start()

    def pair_rows(s, j):
        half_copy(s, j).wait_recv()
        return r.acc[s, half_place(j), :] + r.half_in[s, j].astype(F32)

    def reduce_middle(s):
        for j in far_first:
            r.column_out[s, j - 1] = pair_rows(s, j).astype(BF)
            column_copy(s, j).start()

    def reduce_end(s):
        value = pair_rows(s, 0)
        for j in range(1, nz):
            column_copy(s, j).wait_recv()
            value = value + r.column_in[s, j - 1].astype(F32)
        return value

    def reduce_sent(s):
        for j in range(nz):
            half_copy(s, j).wait_send()
            if j:
                column_copy(s, j).wait_send()

    k_mine, k_other = span(low * half, half, half), span((1 - low) * half, half, half)

    def gram_copy(j):
        if j == 0:
            src, dst = r.token_gram.at[k_other, :], r.gram_got
        elif j < bits:
            src, dst = r.gram_sent.at[j - 1], r.gram_wire.at[j - 1]
        else:
            src, dst = r.gram_full.at[k_mine, :], r.gram_full.at[k_mine, :]
        return remote(src, dst, r.gram_s.at[j], r.gram_r.at[j], flip(0 if j == bits else j))

    def gram_step(j):
        if j == 0:
            r.token_gram[...] = contract_last(tokens[...], tokens[...])
            gram_copy(0).start()
            return
        gram_copy(j - 1).wait_recv()
        if j == 1:
            value = r.token_gram[k_mine, :] + r.gram_got[...]
        elif j <= bits:
            value = r.gram_sent[j - 2] + r.gram_wire[j - 2]
        if j < bits:
            r.gram_sent[j - 1] = value
        elif j == bits:
            r.gram_full[k_mine, :] = value
        if j <= bits:
            gram_copy(j).start()
            return
        high = r.gram_full[...].astype(BF)
        r.gram_parts[0] = high
        r.gram_parts[1] = (r.gram_full[...] - high.astype(F32)).astype(BF)

    lax.fori_loop(0, STEPS, linear_step, 0)
    pair_sum(0, STEPS - 1)
    lax.fori_loop(0, STEPS, lambda i, _: (pair_sum(1, i), 0)[1], 0)
    gram_step(0)
    take_chunks(0, hidden_rows, 0, STEPS)
    reduce_start(0)
    gram_step(1)
    take_chunks(1, tangent_rows, 0, STEPS - 1)
    reduce_middle(0)
    take_chunks(1, tangent_rows, STEPS - 1, STEPS)
    reduce_start(1)
    for j in range(2, bits + 1):
        gram_step(j)

    same = jnp.where(own_row[0:1, :] == own_col, 1.0, 0.0)
    for k, copy in enumerate(task_copies):
        copy.wait_recv()
        same = same + jnp.where(r.task_slots[k, 0:1, :] == own_col, 1.0, 0.0)
    weight = 1.0 / (TASKS * jnp.sum(same, axis=1, keepdims=True))

    value = reduce_end(0)
    r.fresh[0] = (weight * (value - r.targets[...].astype(F32))).astype(BF)
    r.ee[block, :] = r.fresh[0]
    e_copies = spread(1, r.fresh.at[0], r.ee, 0)
    reduce_middle(1)

    def gram_rows(i, _):
        at = chunk(i)
        r.both_gram[...] += contract_first(r.both[at, :], r.both[at, :])
        return 0

    r.both_gram[...] = jnp.zeros(r.both_gram.shape, F32)
    lax.fori_loop(0, STEPS, gram_rows, 0)
    forward(1, r.ee, 0, e_copies)
    value = reduce_end(1)
    first = summed(weight * (value * value))
    r.fresh[1] = (weight * value).astype(BF)
    r.ee[span(count + zz * rows, rows, rows), :] = r.fresh[1]
    t_copies = spread(2, r.fresh.at[1], r.ee, count)
    arrived(e_copies)

    def error_rows(i, kept):
        at = chunk(i)
        errors = r.ee[pl.ds(0, count), :]
        back = contract_last(r.low_down[at, :], errors)
        crossing = contract_last(r.outer_low[at, :], errors)
        tangent = r.full[1, at, :].astype(F32)
        curved = r.second[at, :] * back
        r.curved[at, :] = curved
        r.gate_base[at, :] = r.derivative[at, :] * crossing + curved * tangent
        term = 2.0 * r.both[at, :count].astype(F32) * crossing + curved * tangent * tangent
        return kept + folded(term)

    kept = lax.fori_loop(0, STEPS, error_rows, jnp.zeros((8, count), F32))
    first_part = summed(kept)
    gram_step(bits + 1)

    forward(2, r.ee, count, t_copies)
    def norm_rows(i, kept):
        for step in range(STEPS):
            one = r.ups[step, 1, span(i * 16, 16, 16), :].astype(F32)
            two = r.outer_low[span(step * wide + i * 16, 16, 16), :].astype(F32)
            kept = kept + one * one + two * two
        return kept

    norm = summed(lax.fori_loop(0, wide // 16, norm_rows, jnp.zeros((16, width), F32)))
    arrived(t_copies)

    def gate_step(i, _):
        at = chunk(i)
        back = contract_last(r.low_down[at, :], r.ee[pl.ds(count, count), :])
        r.part[2, at, :] = (r.gate_base[at, :] + r.derivative[at, :] * back).astype(BF)
        first_hop(2, i).start()

        @pl.when(i > 0)
        def _():
            pair_sum(2, i - 1)

        return 0

    r.kept[...] = jnp.zeros(r.kept.shape, F32)
    r.gate_gram[...] = jnp.zeros(r.gate_gram.shape, F32)
    r.carry_gram[...] = jnp.zeros(r.carry_gram.shape, F32)

    def gate_rows(at):
        gate = r.gate[at, :]
        lowered = product(gate, r.gram_parts[0]) + product(gate, r.gram_parts[1])
        carried = (r.derivative[at, :] * lowered).astype(BF)
        r.acc[2] += contract_first(carried, r.low_down[at, :])
        r.gate_gram[...] += contract_first(gate, gate)
        r.carry_gram[...] += contract_first(carried, r.both[at, :])
        r.kept[...] += folded(r.curved[at, :] * lowered * lowered)

    lax.fori_loop(0, STEPS, gate_step, 0)
    pair_sum(2, STEPS - 1)
    take_chunks(2, gate_rows, 0, STEPS)
    head, tail = pl.ds(0, count), pl.ds(count, count)
    r.acc[2] += product(r.both_gram[tail, :].astype(BF), r.ee[...])
    reduce_start(2)

    gram = contract_last(r.ee[...], r.ee[...])
    h_t = summed(r.both_gram[tail, head] * gram[count:, :count])
    change = summed(r.gate_gram[...] * r.token_gram[...]) + 2.0 * h_t
    change = change + summed(r.both_gram[head, head] * gram[:count, :count])
    change = change + summed(r.both_gram[tail, tail] * gram[count:, count:])
    carry = summed(r.carry_gram[:, head] * gram[:count, :count])
    carry = carry + summed(r.carry_gram[:, tail] * gram[:count, count:])
    final = summed(r.kept[...]) + 2.0 * carry

    reduce_middle(2)
    value = reduce_end(2)
    final = final + summed(weight * (value * value))
    index = lax.broadcasted_iota(jnp.int32, (1, 128), 1)
    value = jnp.zeros((1, 128), F32)
    for at, number in enumerate((norm, first + first_part, change, final)):
        value = value + jnp.where(index == at, number, 0.0)
    r.own[...] = value
    number_copies = [
        remote(r.own, r.slots.at[k], r.all_s.at[k], r.all_r.at[k], all_places[k])
        for k in range(n * m - 1)
    ]
    for copy in number_copies:
        copy.start()
    for k, copy in enumerate(number_copies):
        copy.wait_recv()
        value = value + r.slots[k]
    norm, first, change, final = (summed(jnp.where(index == at, value, 0.0)) for at in range(4))
    step = norm / (norm + first)
    keep = first / (norm + first)
    norm_next = keep * keep * norm - 2.0 * keep * step * first + step * step * change
    ratio = norm_next / norm
    curvature = (
        norm_next
        + keep * keep * first
        - 2.0 * keep * step * change
        + step * step * final
        - ratio * norm_next / step
    )
    step_next = norm_next / curvature
    r.sums[0:1, :] = jnp.broadcast_to(step + step_next * (ratio + keep), (1, 128))
    r.sums[1:2, :] = jnp.broadcast_to(-step_next * step, (1, 128))

    def sends_done(i, _):
        for s in range(3):
            first_hop(s, i).wait_send()
            for bit in range(1, bits):
                wire_hop(s, bit, i).wait_send()
            last_hop(s, i).wait_send()
        return 0

    lax.fori_loop(0, STEPS, sends_done, 0)
    for j in range(bits + 1):
        gram_copy(j).wait_send()
    for copy in token_copies + e_copies + t_copies + task_copies + number_copies:
        copy.wait_send()
    for s in range(3):
        reduce_sent(s)


def fused(n, m, tokens, targets, task, up, outer_up, down, outer_down):
    hid, width = up.shape
    rows = tokens.shape[0]
    count, half, nz = n * rows, n * rows // 2, n // 2
    bits = m.bit_length() - 1
    hp = -(-hid // (2 * 16 * STEPS)) * 16 * STEPS
    total = 2 * hp
    vm, dma = pltpu.VMEM, pltpu.SemaphoreType.DMA
    links = max(bits - 1, 1)
    outs = {
        "gate": ((total, count), BF),
        "both": ((total, 2 * count), BF),
        "xx": ((count, width), BF),
        "ee": ((2 * count, width), BF),
        "ups": ((STEPS, 2, total // STEPS, width), BF),
        "outer_low": ((total, width), BF),
        "sums": ((8, 128), F32),
    }
    scratch = {
        "low_down": vm((total, width), BF),
        "part": vm((3, total, count), BF),
        "got": vm((3, hp, count), BF),
        "sent": vm((3, links, hp, count), BF),
        "wire": vm((3, links, hp, count), BF),
        "full": vm((2, total, count), BF),
        "derivative": vm((total, count), F32),
        "second": vm((total, count), F32),
        "curved": vm((total, count), F32),
        "gate_base": vm((total, count), F32),
        "acc": vm((3, count, width), F32),
        "half_out": vm((3, half, width), BF),
        "half_in": vm((3, nz, rows, width), BF),
        "column_out": vm((3, nz - 1, rows, width), BF),
        "column_in": vm((3, nz - 1, rows, width), BF),
        "fresh": vm((2, rows, width), BF),
        "token_gram": vm((count, count), F32),
        "gram_got": vm((half, count), F32),
        "gram_sent": vm((links, half, count), F32),
        "gram_wire": vm((links, half, count), F32),
        "gram_full": vm((count, count), F32),
        "gram_parts": vm((2, count, count), BF),
        "both_gram": vm((2 * count, 2 * count), F32),
        "gate_gram": vm((count, count), F32),
        "carry_gram": vm((count, 2 * count), F32),
        "kept": vm((8, count), F32),
        "tokens": vm(tokens.shape, BF),
        "targets": vm(targets.shape, BF),
        "task": pltpu.SMEM(task.shape, task.dtype),
        "task_own": vm((8, 128), F32),
        "task_slots": vm((n - 1, 8, 128), F32),
        "own": vm((1, 128), F32),
        "slots": vm((n * m - 1, 1, 128), F32),
        "small_sem": dma((3,)),
        "load_sem": dma((4, STEPS)),
        "task_s": dma((n - 1,)),
        "task_r": dma((n - 1,)),
        "sp_zs": dma((3, nz - 1)),
        "sp_zr": dma((3, nz - 1)),
        "sp_xs": dma((3, nz)),
        "sp_xr": dma((3, nz)),
        "ex_s": dma((3, bits + 1, STEPS)),
        "ex_r": dma((3, bits + 1, STEPS)),
        "rx_s": dma((3, nz)),
        "rx_r": dma((3, nz)),
        "rz_s": dma((3, nz - 1)),
        "rz_r": dma((3, nz - 1)),
        "gram_s": dma((bits + 1,)),
        "gram_r": dma((bits + 1,)),
        "all_s": dma((n * m - 1,)),
        "all_r": dma((n * m - 1,)),
    }
    inputs = ("task_in", "tokens_in", "targets_in", "up", "outer_up", "down", "outer_down")
    arrays = (task, tokens, targets, up, outer_up, down, outer_down)
    whole = pl.BlockSpec(memory_space=pltpu.VMEM)
    return pl.pallas_call(
        functools.partial(fused_kernel, n, m, hid, inputs + tuple(outs) + tuple(scratch)),
        out_shape=[vm(*o) for o in outs.values()],
        in_specs=[pl.BlockSpec(memory_space=pltpu.HBM)] * len(inputs),
        out_specs=[whole] * len(outs),
        scratch_shapes=list(scratch.values()),
        compiler_params=pltpu.CompilerParams(
            collective_id=0, has_side_effects=True, vmem_limit_bytes=VMEM_LIMIT
        ),
    )(*(pltpu.with_memory_space_constraint(a, pltpu.HBM) for a in arrays))


def output_tiles(hid, wide):
    tiles, start = [], 0
    while start < hid:
        size = 64 if start == 0 else wide // 2
        size = min(size, wide - start % wide, hid - start)
        tiles.append((start, size))
        start += size
    return tiles


def output_kernel(
    gate, both, xx, ee, ups, outer_low, sums, meta_up, meta_down, stage, sems
):
    hid, width = meta_up.shape
    of_outer, of_change = sums[0:1, 0:1], sums[1:2, 0:1]
    wide = ups.shape[2]
    copies = []
    for i, (start, size) in enumerate(output_tiles(hid, wide)):
        at, part = pl.ds(start, size), pl.ds(start % wide, size)
        outer = ups[start // wide, 1, part, :].astype(F32)
        stage[0, at, :] = of_outer * outer + of_change * product(gate[at, :], xx[...])
        outer = outer_low[at, :].astype(F32)
        stage[1, at, :] = of_outer * outer + of_change * product(both[at, :], ee[...])
        for k, meta in enumerate((meta_up, meta_down)):
            copies.append(
                pltpu.make_async_copy(stage.at[k, at, :], meta.at[at, :], sems.at[k, i])
            )
            copies[-1].start()
    for copy in copies:
        copy.wait()


def outputs(hid, gate, both, xx, ee, ups, outer_low, sums):
    width = xx.shape[1]
    tiles = len(output_tiles(hid, ups.shape[2]))
    return pl.pallas_call(
        output_kernel,
        out_shape=[jax.ShapeDtypeStruct((hid, width), F32)] * 2,
        in_specs=[pl.BlockSpec(memory_space=pltpu.VMEM)] * 7,
        out_specs=[pl.BlockSpec(memory_space=pltpu.HBM)] * 2,
        scratch_shapes=[
            pltpu.VMEM((2, hid, width), F32),
            pltpu.SemaphoreType.DMA((2, tiles)),
        ],
        compiler_params=pltpu.CompilerParams(vmem_limit_bytes=OUT_LIMIT),
    )(gate, both, xx, ee, ups, outer_low, sums)


def body(n, m, tokens, targets, task_of_token, up_weight, down_weight, outer_up, outer_down):
    results = fused(
        n, m, tokens, targets, task_of_token, up_weight, outer_up, down_weight, outer_down
    )
    return tuple(outputs(up_weight.shape[0], *results))


def solution(mesh):
    placed = tuple(P("dp") if i == 2 else P("dp", "shard") for i in range(7))
    return jax.shard_map(
        functools.partial(body, mesh.shape["dp"], mesh.shape["shard"]),
        mesh=mesh,
        in_specs=placed,
        out_specs=(P("dp", "shard"), P("dp", "shard")),
        check_vma=False,
    )
```

```python
import functools
import types

import jax
import jax.numpy as jnp
from jax import lax
from jax.experimental import pallas as pl
from jax.experimental.pallas import tpu as pltpu
from jax.sharding import PartitionSpec as P

TASKS = 16
STEPS = 4
BF = jnp.bfloat16
F32 = jnp.float32
MESH = pl.DeviceIdType.MESH
VMEM_LIMIT = 44 * 2**20
OUT_LIMIT = 24 * 2**20


def sigmoid_parts(linear_part):
    argument = linear_part.astype(F32)
    logistic = jax.nn.sigmoid(argument)
    derivative = logistic * (1.0 + argument * (1.0 - logistic))
    second_order = logistic * (1.0 - logistic) * (2.0 + argument * (1.0 - 2.0 * logistic))
    return (argument * logistic, derivative, second_order)


def contract_last(left_side, right_side):
    return lax.dot_general(
        left_side, right_side, (((1,), (1,)), ((), ())), preferred_element_type=F32
    )


def contract_first(left_side, right_side):
    return lax.dot_general(
        left_side, right_side, (((0,), (0,)), ((), ())), preferred_element_type=F32
    )


def product(left_side, right_side):
    return jnp.dot(left_side, right_side, preferred_element_type=F32)


def remote(src, dst, send_sem, recv_sem, where):
    return pltpu.make_async_remote_copy(
        src_ref=src,
        dst_ref=dst,
        send_sem=send_sem,
        recv_sem=recv_sem,
        device_id=where,
        device_id_type=MESH,
    )


def summed(term):
    return jnp.sum(jnp.sum(term, axis=1, keepdims=True), axis=0, keepdims=True)


def folded(term):
    return jnp.sum(term.reshape(term.shape[0] // 8, 8, term.shape[1]), axis=0)


def span(start, size, unit):
    return pl.ds(pl.multiple_of(start, unit), size)


def fused_kernel(n, m, hid, names, *refs):
    r = types.SimpleNamespace(**dict(zip(names, refs)))
    rows, width = r.tokens_in.shape
    count, half, nz = n * rows, n * rows // 2, n // 2
    total = r.both.shape[0]
    hp = total // 2
    h = hp // STEPS
    wide = 2 * h
    bits = m.bit_length() - 1
    me = lax.axis_index("dp")
    xx, zz = lax.rem(me, 2), me // 2
    shard = lax.axis_index("shard")
    low = lax.rem(shard, 2)
    partner = {"dp": 2 * zz + 1 - xx}

    def drain(ref, sem):
        pltpu.make_async_copy(ref, ref, sem).wait()

    def across(j):
        to = zz
        for bit in range(nz.bit_length() - 1):
            if j >> bit & 1:
                step = 1 << bit
                to = to + step - 2 * step * lax.rem(zz // step, 2)
        return to

    column = [{"dp": 2 * across(j) + xx} for j in range(nz)]
    far_first = range(nz - 1, 0, -1)
    dp_places = [{"dp": lax.rem(me + k, n)} for k in range(1, n)]
    shard_places = [{"shard": lax.rem(shard + k, m)} for k in range(1, m)]
    all_places = [
        {"dp": lax.rem(me + a, n), "shard": lax.rem(shard + b, m)}
        for a in range(n)
        for b in range(m)
        if a + b
    ]

    def flip(bit):
        step = 1 << bit
        return {"shard": shard + step - 2 * step * lax.rem(shard // step, 2)}

    barrier = pltpu.get_barrier_semaphore()
    for where in all_places:
        pl.semaphore_signal(barrier, inc=1, device_id=where, device_id_type=MESH)
    small = [
        pltpu.make_async_copy(src, dst, r.small_sem.at[i])
        for i, (src, dst) in enumerate(
            ((r.task_in, r.task), (r.tokens_in, r.tokens), (r.targets_in, r.targets))
        )
    ]
    small[1].start()
    small[0].start()

    def load(src, dst, step, index):
        size = min(wide, hid - step * wide)
        return pltpu.make_async_copy(
            src.at[pl.ds(step * wide, size)], dst.at[pl.ds(0, size)], r.load_sem.at[index]
        )

    loads = []
    for step in range(STEPS):
        if step * wide < hid:
            loads.append(load(r.up, r.ups.at[step, 0], step, 0))
            loads.append(load(r.outer_up, r.ups.at[step, 1], step, 1))
    for step in range(STEPS):
        if step * wide < hid:
            loads.append(load(r.down, r.low_down.at[pl.ds(step * wide, wide)], step, 2))
            loads.append(load(r.outer_down, r.outer_low.at[pl.ds(step * wide, wide)], step, 3))
    small[1].wait()
    small[0].wait()
    for copy in loads + small[2:]:
        copy.start()

    block = span(zz * rows, rows, rows)
    r.xx[block, :] = r.tokens[...]
    for step in range(STEPS):
        gap = min(wide, (step + 1) * wide - hid)
        if gap > 0:
            r.ups[step, :, pl.ds(wide - gap, gap), :] = jnp.zeros((2, gap, width), BF)
    if total > hid:
        r.low_down[pl.ds(hid, total - hid), :] = jnp.zeros((total - hid, width), BF)
        r.outer_low[pl.ds(hid, total - hid), :] = jnp.zeros((total - hid, width), BF)
    r.acc[...] = jnp.zeros(r.acc.shape, F32)

    pl.semaphore_wait(barrier, n * m - 1)

    def spread(s, src, dst, offset):
        near = span(offset + zz * rows, rows, rows)
        over = span(offset + half + zz * rows, rows, rows)
        out = [
            remote(src, dst.at[near, :], r.sp_s.at[s], r.sp_zr.at[s, j - 1], column[j])
            for j in far_first
        ]
        out.append(remote(src, dst.at[over, :], r.sp_s.at[s], r.sp_xr.at[s], partner))
        for copy in out:
            copy.start()
        return out

    def forward(s, dst, offset, out):
        for j in range(1, nz):
            out[nz - 1 - j].wait_recv()
            at = span(offset + across(j) * rows, rows, rows)
            over = span(offset + half + across(j) * rows, rows, rows)
            copy = remote(
                dst.at[at, :], dst.at[over, :], r.sp_s.at[s], r.sp_xr.at[s], partner
            )
            copy.start()

    def arrived(s):
        drain(r.xx.at[pl.ds(0, half), :], r.sp_xr.at[s])

    token_copies = spread(0, r.tokens, r.xx, 0)

    lane = lax.broadcasted_iota(jnp.int32, (8, 128), 1)
    line = lax.broadcasted_iota(jnp.int32, (rows, 128), 0)
    own_row = jnp.full((8, 128), -1.0, F32)
    own_col = jnp.zeros((rows, 128), F32)
    for i in range(rows):
        number = r.task[i].astype(F32)
        own_row = jnp.where(lane == i, number, own_row)
        own_col = jnp.where(line == i, number, own_col)
    r.task_own[...] = own_row
    task_copies = [
        remote(r.task_own, r.task_slots.at[k], r.task_s, r.task_r, dp_places[k])
        for k in range(n - 1)
    ]
    for copy in task_copies:
        copy.start()
    forward(0, r.xx, 0, token_copies)
    arrived(0)
    small[2].wait()
    for i in range(4):
        drain(r.low_down.at[pl.ds(0, hid), :], r.load_sem.at[i])
    tokens = r.xx

    def chunk(i):
        return span(i * wide, wide, 16)

    def own_part(i):
        return span(i * wide + low * h, h, 16)

    def strip(i):
        return span(i * h, h, 16)

    full = [r.full.at[0], r.full.at[1], r.full.at[2]]
    pairs = STEPS // 2
    lanes = [slice(0, half), slice(half, count)]

    def side(shape):
        return lax.broadcasted_iota(jnp.int32, shape, 1) < half

    def pack(q, top, bottom):
        if q == 0:
            return jnp.where(side(top.shape), top, pltpu.roll(bottom, half, 1))
        return jnp.where(side(top.shape), pltpu.roll(top, half, 1), bottom)

    def unpack(q, packed):
        turned = pltpu.roll(packed, half, 1)
        return (packed, turned) if q == 0 else (turned, packed)

    def first_hop(s, i):
        away = span(i * wide + (1 - low) * h, h, 16)
        return remote(
            r.part.at[s, away, :], r.got.at[s, strip(i), :], r.ex_s.at[0], r.ex_r.at[s, 0, i], flip(0)
        )

    def wire_hop(s, bit, i):
        return remote(
            r.sent.at[s, bit - 1, strip(i), :],
            r.wire.at[s, bit - 1, strip(i), :],
            r.ex_s.at[bit],
            r.ex_r.at[s, bit, i],
            flip(bit),
        )

    def last_hop(s, i):
        at = own_part(i)
        return remote(
            full[s].at[at, :], full[s].at[at, :], r.ex_s.at[bits], r.ex_r.at[s, bits, i], flip(0)
        )

    def pair_sum(s, i):
        first_hop(s, i).wait_recv()
        value = r.part[s, own_part(i), :].astype(F32) + r.got[s, strip(i), :].astype(F32)
        r.sent[s, 0, strip(i), :] = value.astype(BF)
        wire_hop(s, 1, i).start()

    def take_chunks(s, use, begin, end):
        def step(i, _):
            for bit in range(1, bits):
                wire_hop(s, bit, i).wait_recv()
                value = r.sent[s, bit - 1, strip(i), :].astype(F32)
                value = (value + r.wire[s, bit - 1, strip(i), :].astype(F32)).astype(BF)
                if bit + 1 < bits:
                    r.sent[s, bit, strip(i), :] = value
                    wire_hop(s, bit + 1, i).start()
            full[s][own_part(i), :] = value
            last_hop(s, i).start()

            @pl.when(i > begin)
            def _():
                last_hop(s, i - 1).wait_recv()
                use(i - 1, (1 - low) * h, h)

            use(i, low * h, h)
            return 0

        lax.fori_loop(begin, end, step, 0)
        last_hop(s, end - 1).wait_recv()
        use(end - 1, (1 - low) * h, h)

    def linear_step(p, _):
        parts = []
        for e in range(2):
            i = 2 * p + e
            value = contract_last(r.ups[i].reshape(2 * wide, width), tokens[...])
            r.part[0, chunk(i), :] = value[:wide].astype(BF)
            parts.append(value[wide:])
            first_hop(0, i).start()
            if e:
                pair_sum(0, i - 1)
            else:

                @pl.when(p > 0)
                def _():
                    pair_sum(0, i - 1)

        for q in (1, 0):
            w = p + pairs * (1 - q)
            r.part[1, chunk(w), :] = pack(q, *parts).astype(BF)
            first_hop(1, w).start()
        return 0

    def hidden_rows(i, offset, size):
        at = span(i * wide + offset, size, 16)
        activation, derivative, second_order = sigmoid_parts(r.full[0, at, :])
        hidden = activation.astype(BF)
        r.both[at, count:] = hidden
        r.derivative[at, :] = derivative
        r.second[at, :] = second_order
        r.acc[0] += contract_first(hidden, r.low_down[at, :])
        r.acc[1] += contract_first(hidden, r.outer_low[at, :])

    def unpacked(s, q, first, w, offset, size):
        packed = full[s][span(w * wide + offset, size, 16), :].astype(F32)
        p = w - first
        return [
            (span((2 * p + e) * wide + offset, size, 16), part)
            for e, part in enumerate(unpack(q, packed))
        ]

    def both_rows(ref, ats):
        return jnp.concatenate([ref[at, :] for at in ats], axis=0)

    def tangent_rows(q):
        at_q = lanes[q]

        def use(w, offset, size):
            ats, changes = [], []
            for at, tangent in unpacked(1, q, pairs * (1 - q), w, offset, size):
                change = (r.derivative[at, :] * tangent).astype(BF)
                r.both[at, at_q] = change[:, at_q]
                r.tangent[at, at_q] = tangent[:, at_q].astype(BF)
                ats.append(at)
                changes.append(change)
            change = jnp.concatenate(changes, axis=0)
            r.acc[1, at_q] += contract_first(change, both_rows(r.low_down, ats))[at_q]

        return use

    def half_place(j):
        return span(across(j) * rows, rows, rows)

    def half_copy(s, j):
        return remote(
            r.half_out.at[s, half_place(j), :], r.half_in.at[s, j], r.rx_s.at[s], r.rx_r.at[s, j], partner
        )

    def column_copy(s, j):
        return remote(
            r.column_out.at[s, j - 1], r.column_in.at[s, j - 1], r.rz_s.at[s], r.rz_r.at[s], column[j]
        )

    def reduce_start(s):
        r.half_out[s] = r.acc[s, pl.ds(half, half), :].astype(BF)
        for j in range(nz - 1, -1, -1):
            half_copy(s, j).start()

    def pair_rows(s, j):
        half_copy(s, j).wait_recv()
        return r.acc[s, half_place(j), :] + r.half_in[s, j].astype(F32)

    def reduce_middle(s):
        for j in far_first:
            r.column_out[s, j - 1] = pair_rows(s, j).astype(BF)
            column_copy(s, j).start()

    def reduce_end(s):
        value = pair_rows(s, 0)
        drain(r.column_in.at[s], r.rz_r.at[s])
        for j in range(1, nz):
            value = value + r.column_in[s, j - 1].astype(F32)
        return value

    k_mine, k_other = span(low * half, half, half), span((1 - low) * half, half, half)

    def gram_copy(j):
        if j == 0:
            src, dst = r.token_gram.at[k_other, :], r.gram_got
        elif j < bits:
            src, dst = r.gram_sent.at[j - 1], r.gram_wire.at[j - 1]
        else:
            src, dst = r.gram_full.at[k_mine, :], r.gram_full.at[k_mine, :]
        return remote(src, dst, r.gram_s.at[j], r.gram_r.at[j], flip(0 if j == bits else j))

    def gram_step(j):
        if j == 0:
            r.token_gram[...] = contract_last(tokens[...], tokens[...])
            gram_copy(0).start()
            return
        gram_copy(j - 1).wait_recv()
        if j == 1:
            value = r.token_gram[k_mine, :] + r.gram_got[...]
        elif j <= bits:
            value = r.gram_sent[j - 2] + r.gram_wire[j - 2]
        if j < bits:
            r.gram_sent[j - 1] = value
        elif j == bits:
            r.gram_full[k_mine, :] = value
        if j <= bits:
            gram_copy(j).start()
            return
        high = r.gram_full[...].astype(BF)
        r.gram_parts[:, :count] = high
        r.gram_parts[:, count:] = (r.gram_full[...] - high.astype(F32)).astype(BF)

    lax.fori_loop(0, pairs, linear_step, 0)
    pair_sum(0, STEPS - 1)
    lax.fori_loop(0, STEPS, lambda i, _: (pair_sum(1, i), 0)[1], 0)
    gram_step(0)
    take_chunks(0, hidden_rows, 0, STEPS)
    reduce_start(0)
    gram_step(1)
    take_chunks(1, tangent_rows(1), 0, pairs)
    reduce_start(1)
    reduce_middle(0)
    take_chunks(1, tangent_rows(0), pairs, STEPS)
    reduce_middle(1)
    for j in range(2, bits + 1):
        gram_step(j)

    same = jnp.where(own_row[0:1, :] == own_col, 1.0, 0.0)
    drain(r.task_slots, r.task_r)
    for k in range(n - 1):
        same = same + jnp.where(r.task_slots[k, 0:1, :] == own_col, 1.0, 0.0)
    weight = 1.0 / (TASKS * jnp.sum(same, axis=1, keepdims=True))

    value = reduce_end(0)
    r.fresh[0] = (weight * (value - r.targets[...].astype(F32))).astype(BF)
    r.ee[block, :] = r.fresh[0]
    e_copies = spread(1, r.fresh.at[0], r.ee, 0)

    def gram_rows(i, _):
        at = chunk(i)
        r.both_gram[...] += contract_first(r.both[at, :], r.both[at, :])
        return 0

    r.both_gram[...] = jnp.zeros(r.both_gram.shape, F32)
    lax.fori_loop(0, STEPS, gram_rows, 0)

    def norm_rows(i, kept):
        for step in range(STEPS):
            one = r.ups[step, 1, span(i * 16, 16, 16), :].astype(F32)
            two = r.outer_low[span(step * wide + i * 16, 16, 16), :].astype(F32)
            kept = kept + one * one + two * two
        return kept

    norm = summed(lax.fori_loop(0, wide // 16, norm_rows, jnp.zeros((16, width), F32)))
    gram_step(bits + 1)
    value = reduce_end(1)
    first = summed(weight * (value * value))
    r.fresh[1] = (weight * value).astype(BF)
    r.ee[span(count + zz * rows, rows, rows), :] = r.fresh[1]
    t_copies = spread(2, r.fresh.at[1], r.ee, count)
    forward(1, r.ee, 0, e_copies)

    own, over = lanes

    def own_error_rows(i, _):
        at = chunk(i)
        errors = r.ee[pl.ds(0, half), :]
        back = contract_last(r.low_down[at, :], errors)
        crossing = contract_last(r.outer_low[at, :], errors)
        curved = r.second[at, own] * back
        r.curved[at, own] = curved
        tangent = r.tangent[at, own].astype(F32)
        r.gate_base[at, own] = r.derivative[at, own] * crossing + curved * tangent
        return 0

    def over_error_rows(i, kept):
        at = chunk(i)
        crossing = contract_last(r.outer_low[at, :], r.ee[pl.ds(0, count), :])
        tangent, curved = r.tangent[at, :].astype(F32), r.curved[at, :]
        value = r.derivative[at, :] * crossing + curved * tangent
        r.gate_base[at, over] = value[:, over]
        term = 2.0 * r.both[at, :count].astype(F32) * crossing + curved * tangent * tangent
        return kept + folded(term)

    def gate_pair(q, p):
        at = span(2 * p * wide, 2 * wide, 16)
        w = p + pairs * q
        if q == 0:
            back = contract_last(r.low_down[at, :], r.ee[pl.ds(half, count), :])
            back = pltpu.roll(back, half, 1)
            r.curved[at, over] = r.second[at, over] * back[:, over]
            value = r.gate_base[at, own] + r.derivative[at, own] * back[:, own]
            packed = jnp.concatenate([value[:wide], value[wide:]], axis=1)
        else:
            back = contract_last(r.low_down[at, :], r.ee[pl.ds(count, count), :])
            value = r.gate_base[at, :] + r.derivative[at, :] * back
            packed = pack(1, value[:wide], value[wide:])
        r.part[2, chunk(w), :] = packed.astype(BF)
        first_hop(2, w).start()

    def gate_side(q):
        for p in range(pairs):
            gate_pair(q, p)
            if p:
                pair_sum(2, pairs * q + p - 1)

    def gate_rows(q):
        at_q = lanes[q]

        def use(w, offset, size):
            ats = []
            for at, part in unpacked(2, q, pairs * q, w, offset, size):
                r.gate[at, at_q] = part[:, at_q].astype(BF)
                ats.append(at)
            if q == 0:
                return
            lowered = product(both_rows(r.gate, ats), r.gram_parts[...])
            lowered = lowered[:, :count] + lowered[:, count:]
            carried = (both_rows(r.derivative, ats) * lowered).astype(BF)
            r.acc[2] += contract_first(carried, both_rows(r.low_down, ats))
            for k, at in enumerate(ats):
                r.carried[at, :] = carried[k * size : (k + 1) * size]
            r.kept[...] += folded(both_rows(r.curved, ats) * lowered * lowered)

        return use

    r.kept[...] = jnp.zeros(r.kept.shape, F32)
    r.gate_gram[...] = jnp.zeros(r.gate_gram.shape, F32)
    r.carry_gram[...] = jnp.zeros(r.carry_gram.shape, F32)
    lax.fori_loop(0, STEPS, own_error_rows, 0)
    forward(2, r.ee, count, t_copies)
    arrived(1)
    gate_side(0)
    kept = over_error_rows(0, jnp.zeros((8, count), F32))
    pair_sum(2, pairs - 1)
    kept = lax.fori_loop(1, STEPS, over_error_rows, kept)
    arrived(2)
    gate_side(1)
    first_part = summed(kept)
    head, tail = pl.ds(0, count), pl.ds(count, count)
    r.acc[2] = product(r.both_gram[tail, :].astype(BF), r.ee[...])
    gram = contract_last(r.ee[...], r.ee[...])
    h_t = summed(r.both_gram[tail, head] * gram[count:, :count])
    change = 2.0 * h_t + summed(r.both_gram[head, head] * gram[:count, :count])
    change = change + summed(r.both_gram[tail, tail] * gram[count:, count:])
    r.error_gram[...] = gram[:count, :]
    pair_sum(2, STEPS - 1)
    take_chunks(2, gate_rows(0), 0, pairs)
    take_chunks(2, gate_rows(1), pairs, STEPS)
    reduce_start(2)

    def late_rows(i, _):
        at = chunk(i)
        gate = r.gate[at, :]
        r.gate_gram[...] += contract_first(gate, gate)
        r.carry_gram[...] += contract_first(r.carried[at, :], r.both[at, :])
        return 0

    lax.fori_loop(0, STEPS, late_rows, 0)
    change = change + summed(r.gate_gram[...] * r.token_gram[...])
    carry = summed(r.carry_gram[...] * r.error_gram[...])
    final = summed(r.kept[...]) + 2.0 * carry
    reduce_middle(2)
    value = reduce_end(2)
    final = final + summed(weight * (value * value))
    index = lax.broadcasted_iota(jnp.int32, (1, 128), 1)
    value = jnp.zeros((1, 128), F32)
    for at, number in enumerate((norm, first + first_part, change, final)):
        value = value + jnp.where(index == at, number, 0.0)
    r.own[...] = value
    number_copies = [
        remote(r.own, r.slots.at[k], r.all_s, r.all_r, all_places[k])
        for k in range(n * m - 1)
    ]
    for copy in number_copies:
        copy.start()
    drain(r.slots, r.all_r)
    for k in range(n * m - 1):
        value = value + r.slots[k]
    norm, first, change, final = (summed(jnp.where(index == at, value, 0.0)) for at in range(4))
    step = norm / (norm + first)
    keep = first / (norm + first)
    norm_next = keep * keep * norm - 2.0 * keep * step * first + step * step * change
    ratio = norm_next / norm
    curvature = (
        norm_next
        + keep * keep * first
        - 2.0 * keep * step * change
        + step * step * final
        - ratio * norm_next / step
    )
    step_next = norm_next / curvature
    r.sums[0:1, :] = jnp.broadcast_to(step + step_next * (ratio + keep), (1, 128))
    r.sums[1:2, :] = jnp.broadcast_to(-step_next * step, (1, 128))

    for hop in range(bits + 1):
        drain(r.got, r.ex_s.at[hop])
        gram_copy(hop).wait_send()
    for k in range(3):
        drain(r.xx.at[pl.ds(0, (n - 1) * rows), :], r.sp_s.at[k])
        drain(r.half_out.at[k], r.rx_s.at[k])
        drain(r.column_out.at[k], r.rz_s.at[k])
    drain(r.task_slots, r.task_s)
    drain(r.slots, r.all_s)


def fused(n, m, tokens, targets, task, up, outer_up, down, outer_down):
    hid, width = up.shape
    rows = tokens.shape[0]
    count, half, nz = n * rows, n * rows // 2, n // 2
    bits = m.bit_length() - 1
    hp = -(-hid // (2 * 16 * STEPS)) * 16 * STEPS
    total = 2 * hp
    vm, dma = pltpu.VMEM, pltpu.SemaphoreType.DMA
    links = max(bits - 1, 1)
    outs = {
        "gate": ((total, count), BF),
        "both": ((total, 2 * count), BF),
        "xx": ((count, width), BF),
        "ee": ((2 * count, width), BF),
        "ups": ((STEPS, 2, total // STEPS, width), BF),
        "outer_low": ((total, width), BF),
        "sums": ((8, 128), F32),
    }
    scratch = {
        "low_down": vm((total, width), BF),
        "part": vm((3, total, count), BF),
        "got": vm((3, hp, count), BF),
        "sent": vm((3, links, hp, count), BF),
        "wire": vm((3, links, hp, count), BF),
        "full": vm((3, total, count), BF),
        "tangent": vm((total, count), BF),
        "derivative": vm((total, count), F32),
        "second": vm((total, count), F32),
        "curved": vm((total, count), F32),
        "gate_base": vm((total, count), F32),
        "acc": vm((3, count, width), F32),
        "half_out": vm((3, half, width), BF),
        "half_in": vm((3, nz, rows, width), BF),
        "column_out": vm((3, nz - 1, rows, width), BF),
        "column_in": vm((3, nz - 1, rows, width), BF),
        "fresh": vm((2, rows, width), BF),
        "token_gram": vm((count, count), F32),
        "gram_got": vm((half, count), F32),
        "gram_sent": vm((links, half, count), F32),
        "gram_wire": vm((links, half, count), F32),
        "gram_full": vm((count, count), F32),
        "gram_parts": vm((count, 2 * count), BF),
        "both_gram": vm((2 * count, 2 * count), F32),
        "gate_gram": vm((count, count), F32),
        "carry_gram": vm((count, 2 * count), F32),
        "error_gram": vm((count, 2 * count), F32),
        "carried": vm((total, count), BF),
        "kept": vm((8, count), F32),
        "tokens": vm(tokens.shape, BF),
        "targets": vm(targets.shape, BF),
        "task": pltpu.SMEM(task.shape, task.dtype),
        "task_own": vm((8, 128), F32),
        "task_slots": vm((n - 1, 8, 128), F32),
        "own": vm((1, 128), F32),
        "slots": vm((n * m - 1, 1, 128), F32),
        "small_sem": dma((3,)),
        "load_sem": dma((4,)),
        "task_s": dma,
        "task_r": dma,
        "sp_s": dma((3,)),
        "sp_zr": dma((3, nz - 1)),
        "sp_xr": dma((3,)),
        "ex_s": dma((bits + 1,)),
        "ex_r": dma((3, bits + 1, STEPS)),
        "rx_s": dma((3,)),
        "rx_r": dma((3, nz)),
        "rz_s": dma((3,)),
        "rz_r": dma((3,)),
        "gram_s": dma((bits + 1,)),
        "gram_r": dma((bits + 1,)),
        "all_s": dma,
        "all_r": dma,
    }
    inputs = ("task_in", "tokens_in", "targets_in", "up", "outer_up", "down", "outer_down")
    arrays = (task, tokens, targets, up, outer_up, down, outer_down)
    whole = pl.BlockSpec(memory_space=pltpu.VMEM)
    return pl.pallas_call(
        functools.partial(fused_kernel, n, m, hid, inputs + tuple(outs) + tuple(scratch)),
        out_shape=[vm(*o) for o in outs.values()],
        in_specs=[pl.BlockSpec(memory_space=pltpu.HBM)] * len(inputs),
        out_specs=[whole] * len(outs),
        scratch_shapes=list(scratch.values()),
        compiler_params=pltpu.CompilerParams(
            collective_id=0, has_side_effects=True, vmem_limit_bytes=VMEM_LIMIT
        ),
    )(*(pltpu.with_memory_space_constraint(a, pltpu.HBM) for a in arrays))


def output_tiles(hid, wide):
    tiles, start = [], 0
    while start < hid:
        size = 64 if start == 0 else wide // 2
        size = min(size, wide - start % wide, hid - start)
        tiles.append((start, size))
        start += size
    return tiles


def output_kernel(
    gate, both, xx, ee, ups, outer_low, sums, meta_up, meta_down, stage, sems
):
    hid, width = meta_up.shape
    of_outer, of_change = sums[0:1, 0:1], sums[1:2, 0:1]
    wide = ups.shape[2]
    for start, size in output_tiles(hid, wide):
        at, part = pl.ds(start, size), pl.ds(start % wide, size)
        outer = ups[start // wide, 1, part, :].astype(F32)
        stage[0, at, :] = of_outer * outer + of_change * product(gate[at, :], xx[...])
        outer = outer_low[at, :].astype(F32)
        stage[1, at, :] = of_outer * outer + of_change * product(both[at, :], ee[...])
        for k, meta in enumerate((meta_up, meta_down)):
            pltpu.make_async_copy(stage.at[k, at, :], meta.at[at, :], sems.at[k]).start()
    for k, meta in enumerate((meta_up, meta_down)):
        pltpu.make_async_copy(stage.at[k], meta, sems.at[k]).wait()


def outputs(hid, gate, both, xx, ee, ups, outer_low, sums):
    width = xx.shape[1]
    return pl.pallas_call(
        output_kernel,
        out_shape=[jax.ShapeDtypeStruct((hid, width), F32)] * 2,
        in_specs=[pl.BlockSpec(memory_space=pltpu.VMEM)] * 7,
        out_specs=[pl.BlockSpec(memory_space=pltpu.HBM)] * 2,
        scratch_shapes=[
            pltpu.VMEM((2, hid, width), F32),
            pltpu.SemaphoreType.DMA((2,)),
        ],
        compiler_params=pltpu.CompilerParams(vmem_limit_bytes=OUT_LIMIT),
    )(gate, both, xx, ee, ups, outer_low, sums)


def body(n, m, tokens, targets, task_of_token, up_weight, down_weight, outer_up, outer_down):
    results = fused(
        n, m, tokens, targets, task_of_token, up_weight, outer_up, down_weight, outer_down
    )
    return tuple(outputs(up_weight.shape[0], *results))


def solution(mesh):
    placed = tuple(P("dp") if i == 2 else P("dp", "shard") for i in range(7))
    return jax.shard_map(
        functools.partial(body, mesh.shape["dp"], mesh.shape["shard"]),
        mesh=mesh,
        in_specs=placed,
        out_specs=(P("dp", "shard"), P("dp", "shard")),
        check_vma=False,
    )
```

```python
import functools
import types

import jax
import jax.numpy as jnp
from jax import lax
from jax.experimental import pallas as pl
from jax.experimental.pallas import tpu as pltpu
from jax.sharding import PartitionSpec as P

TASKS = 16
STEPS = 4
BF = jnp.bfloat16
F32 = jnp.float32
MESH = pl.DeviceIdType.MESH
VMEM_LIMIT = 44 * 2**20
OUT_LIMIT = 24 * 2**20


def sigmoid_parts(linear_part):
    argument = linear_part.astype(F32)
    logistic = jax.nn.sigmoid(argument)
    derivative = logistic * (1.0 + argument * (1.0 - logistic))
    second_order = logistic * (1.0 - logistic) * (2.0 + argument * (1.0 - 2.0 * logistic))
    return (argument * logistic, derivative, second_order)


def contract_last(left_side, right_side):
    return lax.dot_general(
        left_side, right_side, (((1,), (1,)), ((), ())), preferred_element_type=F32
    )


def contract_first(left_side, right_side):
    return lax.dot_general(
        left_side, right_side, (((0,), (0,)), ((), ())), preferred_element_type=F32
    )


def product(left_side, right_side):
    return jnp.dot(left_side, right_side, preferred_element_type=F32)


def remote(src, dst, send_sem, recv_sem, where):
    return pltpu.make_async_remote_copy(
        src_ref=src,
        dst_ref=dst,
        send_sem=send_sem,
        recv_sem=recv_sem,
        device_id=where,
        device_id_type=MESH,
    )


def summed(term):
    return jnp.sum(jnp.sum(term, axis=1, keepdims=True), axis=0, keepdims=True)


def folded(term):
    return jnp.sum(term.reshape(term.shape[0] // 8, 8, term.shape[1]), axis=0)


def span(start, size, unit):
    return pl.ds(pl.multiple_of(start, unit), size)


def fused_kernel(n, m, hid, names, *refs):
    r = types.SimpleNamespace(**dict(zip(names, refs)))
    rows, width = r.tokens_in.shape
    count, half, nz = n * rows, n * rows // 2, n // 2
    total = r.both.shape[0]
    hp = total // 2
    h = hp // STEPS
    wide = 2 * h
    bits = m.bit_length() - 1
    me = lax.axis_index("dp")
    xx, zz = lax.rem(me, 2), me // 2
    shard = lax.axis_index("shard")
    low = lax.rem(shard, 2)
    partner = {"dp": 2 * zz + 1 - xx}

    def drain(ref, sem):
        pltpu.make_async_copy(ref, ref, sem).wait()

    def across(j):
        to = zz
        for bit in range(nz.bit_length() - 1):
            if j >> bit & 1:
                step = 1 << bit
                to = to + step - 2 * step * lax.rem(zz // step, 2)
        return to

    column = [{"dp": 2 * across(j) + xx} for j in range(nz)]
    far_first = range(nz - 1, 0, -1)
    dp_places = [{"dp": lax.rem(me + k, n)} for k in range(1, n)]
    shard_places = [{"shard": lax.rem(shard + k, m)} for k in range(1, m)]
    all_places = [
        {"dp": lax.rem(me + a, n), "shard": lax.rem(shard + b, m)}
        for a in range(n)
        for b in range(m)
        if a + b
    ]

    def flip(bit):
        step = 1 << bit
        return {"shard": shard + step - 2 * step * lax.rem(shard // step, 2)}

    barrier = pltpu.get_barrier_semaphore()
    for where in all_places:
        pl.semaphore_signal(barrier, inc=1, device_id=where, device_id_type=MESH)
    small = [
        pltpu.make_async_copy(src, dst, r.small_sem.at[i])
        for i, (src, dst) in enumerate(
            ((r.task_in, r.task), (r.tokens_in, r.tokens), (r.targets_in, r.targets))
        )
    ]
    small[1].start()
    small[0].start()

    def load(src, dst, step, index):
        size = min(wide, hid - step * wide)
        return pltpu.make_async_copy(
            src.at[pl.ds(step * wide, size)], dst.at[pl.ds(0, size)], r.load_sem.at[index]
        )

    loads = []
    for step in range(STEPS):
        if step * wide < hid:
            loads.append(load(r.up, r.ups.at[step, 0], step, 0))
            loads.append(load(r.outer_up, r.ups.at[step, 1], step, 1))
    for step in range(STEPS):
        if step * wide < hid:
            loads.append(load(r.down, r.low_down.at[pl.ds(step * wide, wide)], step, 2))
            loads.append(load(r.outer_down, r.outer_low.at[pl.ds(step * wide, wide)], step, 3))
    small[1].wait()
    small[0].wait()
    for copy in loads + small[2:]:
        copy.start()

    block = span(zz * rows, rows, rows)
    r.xx[block, :] = r.tokens[...]
    for step in range(STEPS):
        gap = min(wide, (step + 1) * wide - hid)
        if gap > 0:
            r.ups[step, :, pl.ds(wide - gap, gap), :] = jnp.zeros((2, gap, width), BF)
    if total > hid:
        r.low_down[pl.ds(hid, total - hid), :] = jnp.zeros((total - hid, width), BF)
        r.outer_low[pl.ds(hid, total - hid), :] = jnp.zeros((total - hid, width), BF)
    r.acc[...] = jnp.zeros(r.acc.shape, F32)

    pl.semaphore_wait(barrier, n * m - 1)

    def spread(s, src, dst, offset):
        near = span(offset + zz * rows, rows, rows)
        over = span(offset + half + zz * rows, rows, rows)
        out = [
            remote(src, dst.at[near, :], r.sp_s.at[s], r.sp_zr.at[s, j - 1], column[j])
            for j in far_first
        ]
        out.append(remote(src, dst.at[over, :], r.sp_s.at[s], r.sp_xr.at[s], partner))
        for copy in out:
            copy.start()
        return out

    def forward(s, dst, offset, out):
        for j in range(1, nz):
            out[nz - 1 - j].wait_recv()
            at = span(offset + across(j) * rows, rows, rows)
            over = span(offset + half + across(j) * rows, rows, rows)
            copy = remote(
                dst.at[at, :], dst.at[over, :], r.sp_s.at[s], r.sp_xr.at[s], partner
            )
            copy.start()

    def arrived(s):
        drain(r.xx.at[pl.ds(0, half), :], r.sp_xr.at[s])

    token_copies = spread(0, r.tokens, r.xx, 0)

    lane = lax.broadcasted_iota(jnp.int32, (8, 128), 1)
    line = lax.broadcasted_iota(jnp.int32, (rows, 128), 0)
    own_row = jnp.full((8, 128), -1.0, F32)
    own_col = jnp.zeros((rows, 128), F32)
    for i in range(rows):
        number = r.task[i].astype(F32)
        own_row = jnp.where(lane == i, number, own_row)
        own_col = jnp.where(line == i, number, own_col)
    r.task_own[...] = own_row
    task_copies = [
        remote(r.task_own, r.task_slots.at[k], r.task_s, r.task_r, dp_places[k])
        for k in range(n - 1)
    ]
    for copy in task_copies:
        copy.start()
    forward(0, r.xx, 0, token_copies)
    arrived(0)
    small[2].wait()
    for i in range(4):
        drain(r.low_down.at[pl.ds(0, hid), :], r.load_sem.at[i])
    tokens = r.xx

    def chunk(i):
        return span(i * wide, wide, 16)

    def own_part(i):
        return span(i * wide + low * h, h, 16)

    def strip(i):
        return span(i * h, h, 16)

    full = [r.full.at[0], r.full.at[1], r.full.at[2]]
    pairs = STEPS // 2
    lanes = [slice(0, half), slice(half, count)]

    def side(shape):
        return lax.broadcasted_iota(jnp.int32, shape, 1) < half

    def pack(q, top, bottom):
        if q == 0:
            return jnp.where(side(top.shape), top, pltpu.roll(bottom, half, 1))
        return jnp.where(side(top.shape), pltpu.roll(top, half, 1), bottom)

    def unpack(q, packed):
        turned = pltpu.roll(packed, half, 1)
        return (packed, turned) if q == 0 else (turned, packed)

    def first_hop(s, i):
        away = span(i * wide + (1 - low) * h, h, 16)
        return remote(
            r.part.at[s, away, :], r.got.at[s, strip(i), :], r.ex_s.at[0], r.ex_r.at[s, 0, i], flip(0)
        )

    def wire_hop(s, bit, i):
        return remote(
            r.sent.at[s, bit - 1, strip(i), :],
            r.wire.at[s, bit - 1, strip(i), :],
            r.ex_s.at[bit],
            r.ex_r.at[s, bit, i],
            flip(bit),
        )

    def last_hop(s, i):
        at = own_part(i)
        return remote(
            full[s].at[at, :], full[s].at[at, :], r.ex_s.at[bits], r.ex_r.at[s, bits, i], flip(0)
        )

    def pair_sum(s, i):
        first_hop(s, i).wait_recv()
        value = r.part[s, own_part(i), :].astype(F32) + r.got[s, strip(i), :].astype(F32)
        r.sent[s, 0, strip(i), :] = value.astype(BF)
        wire_hop(s, 1, i).start()

    def take_chunks(s, use, begin, end, prompt=False):
        def step(i, _):
            for bit in range(1, bits):
                wire_hop(s, bit, i).wait_recv()
                value = r.sent[s, bit - 1, strip(i), :].astype(F32)
                value = (value + r.wire[s, bit - 1, strip(i), :].astype(F32)).astype(BF)
                if bit + 1 < bits:
                    r.sent[s, bit, strip(i), :] = value
                    wire_hop(s, bit + 1, i).start()
            full[s][own_part(i), :] = value
            last_hop(s, i).start()
            if prompt:
                use(i, low * h, h)
                last_hop(s, i).wait_recv()
                use(i, (1 - low) * h, h)
                return 0

            @pl.when(i > begin)
            def _():
                last_hop(s, i - 1).wait_recv()
                use(i - 1, (1 - low) * h, h)

            use(i, low * h, h)
            return 0

        lax.fori_loop(begin, end, step, 0)
        if not prompt:
            last_hop(s, end - 1).wait_recv()
            use(end - 1, (1 - low) * h, h)

    def linear_step(p, _):
        parts = []
        for e in range(2):
            i = 2 * p + e
            value = contract_last(r.ups[i].reshape(2 * wide, width), tokens[...])
            r.part[0, chunk(i), :] = value[:wide].astype(BF)
            parts.append(value[wide:])
            first_hop(0, i).start()
            if e:
                pair_sum(0, i - 1)
            else:

                @pl.when(p > 0)
                def _():
                    pair_sum(0, i - 1)

        for q in (1, 0):
            w = p + pairs * (1 - q)
            r.part[1, chunk(w), :] = pack(q, *parts).astype(BF)
            first_hop(1, w).start()
        return 0

    def hidden_rows(i, offset, size):
        at = span(i * wide + offset, size, 16)
        activation, derivative, second_order = sigmoid_parts(r.full[0, at, :])
        hidden = activation.astype(BF)
        r.both[at, count:] = hidden
        r.derivative[at, :] = derivative
        r.second[at, :] = second_order
        r.acc[0] += contract_first(hidden, r.low_down[at, :])
        r.acc[1] += contract_first(hidden, r.outer_low[at, :])

    def unpacked(s, q, first, w, offset, size):
        packed = full[s][span(w * wide + offset, size, 16), :].astype(F32)
        p = w - first
        return [
            (span((2 * p + e) * wide + offset, size, 16), part)
            for e, part in enumerate(unpack(q, packed))
        ]

    def both_rows(ref, ats):
        return jnp.concatenate([ref[at, :] for at in ats], axis=0)

    def tangent_rows(q):
        at_q = lanes[q]

        def use(w, offset, size):
            ats, changes = [], []
            for at, tangent in unpacked(1, q, pairs * (1 - q), w, offset, size):
                change = (r.derivative[at, :] * tangent).astype(BF)
                r.both[at, at_q] = change[:, at_q]
                r.tangent[at, at_q] = tangent[:, at_q].astype(BF)
                ats.append(at)
                changes.append(change)
            change = jnp.concatenate(changes, axis=0)
            r.acc[1, at_q] += contract_first(change, both_rows(r.low_down, ats))[at_q]

        return use

    def half_place(j):
        return span(across(j) * rows, rows, rows)

    def half_copy(s, j):
        return remote(
            r.half_out.at[s, half_place(j), :], r.half_in.at[s, j], r.rx_s.at[s], r.rx_r.at[s, j], partner
        )

    def column_copy(s, j):
        return remote(
            r.column_out.at[s, j - 1], r.column_in.at[s, j - 1], r.rz_s.at[s], r.rz_r.at[s], column[j]
        )

    def reduce_start(s):
        r.half_out[s] = r.acc[s, pl.ds(half, half), :].astype(BF)
        for j in range(nz - 1, -1, -1):
            half_copy(s, j).start()

    def pair_rows(s, j):
        half_copy(s, j).wait_recv()
        return r.acc[s, half_place(j), :] + r.half_in[s, j].astype(F32)

    def reduce_middle(s):
        for j in far_first:
            r.column_out[s, j - 1] = pair_rows(s, j).astype(BF)
            column_copy(s, j).start()

    def reduce_end(s):
        value = pair_rows(s, 0)
        drain(r.column_in.at[s], r.rz_r.at[s])
        for j in range(1, nz):
            value = value + r.column_in[s, j - 1].astype(F32)
        return value

    k_mine, k_other = span(low * half, half, half), span((1 - low) * half, half, half)

    def gram_copy(j):
        if j == 0:
            src, dst = r.token_gram.at[k_other, :], r.gram_got
        elif j < bits:
            src, dst = r.gram_sent.at[j - 1], r.gram_wire.at[j - 1]
        else:
            src, dst = r.gram_full.at[k_mine, :], r.gram_full.at[k_mine, :]
        return remote(src, dst, r.gram_s.at[j], r.gram_r.at[j], flip(0 if j == bits else j))

    def gram_step(j):
        if j == 0:
            r.token_gram[...] = contract_last(tokens[...], tokens[...])
            gram_copy(0).start()
            return
        gram_copy(j - 1).wait_recv()
        if j == 1:
            value = r.token_gram[k_mine, :] + r.gram_got[...]
        elif j <= bits:
            value = r.gram_sent[j - 2] + r.gram_wire[j - 2]
        if j < bits:
            r.gram_sent[j - 1] = value
        elif j == bits:
            r.gram_full[k_mine, :] = value
        if j <= bits:
            gram_copy(j).start()
            return
        high = r.gram_full[...].astype(BF)
        r.gram_parts[:, :count] = high
        r.gram_parts[:, count:] = (r.gram_full[...] - high.astype(F32)).astype(BF)

    lax.fori_loop(0, pairs, linear_step, 0)
    pair_sum(0, STEPS - 1)
    lax.fori_loop(0, STEPS, lambda i, _: (pair_sum(1, i), 0)[1], 0)
    gram_step(0)
    take_chunks(0, hidden_rows, 0, STEPS)
    reduce_start(0)
    gram_step(1)
    take_chunks(1, tangent_rows(1), 0, pairs)
    reduce_start(1)
    reduce_middle(0)
    take_chunks(1, tangent_rows(0), pairs, STEPS)
    reduce_middle(1)
    for j in range(2, bits + 1):
        gram_step(j)

    same = jnp.where(own_row[0:1, :] == own_col, 1.0, 0.0)
    drain(r.task_slots, r.task_r)
    for k in range(n - 1):
        same = same + jnp.where(r.task_slots[k, 0:1, :] == own_col, 1.0, 0.0)
    weight = 1.0 / (TASKS * jnp.sum(same, axis=1, keepdims=True))

    value = reduce_end(0)
    r.fresh[0] = (weight * (value - r.targets[...].astype(F32))).astype(BF)
    r.ee[block, :] = r.fresh[0]
    e_copies = spread(1, r.fresh.at[0], r.ee, 0)

    def gram_rows(i, _):
        at = chunk(i)
        r.both_gram[...] += contract_first(r.both[at, :], r.both[at, :])
        return 0

    r.both_gram[...] = jnp.zeros(r.both_gram.shape, F32)
    lax.fori_loop(0, STEPS, gram_rows, 0)

    def norm_rows(i, kept):
        for step in range(STEPS):
            one = r.ups[step, 1, span(i * 16, 16, 16), :].astype(F32)
            two = r.outer_low[span(step * wide + i * 16, 16, 16), :].astype(F32)
            kept = kept + one * one + two * two
        return kept

    norm = summed(lax.fori_loop(0, wide // 16, norm_rows, jnp.zeros((16, width), F32)))
    gram_step(bits + 1)
    value = reduce_end(1)
    first = summed(weight * (value * value))
    r.fresh[1] = (weight * value).astype(BF)
    r.ee[span(count + zz * rows, rows, rows), :] = r.fresh[1]
    t_copies = spread(2, r.fresh.at[1], r.ee, count)
    forward(1, r.ee, 0, e_copies)

    own, over = lanes

    def own_error_rows(i, _):
        at = chunk(i)
        errors = r.ee[pl.ds(0, half), :]
        back = contract_last(r.low_down[at, :], errors)
        crossing = contract_last(r.outer_low[at, :], errors)
        curved = r.second[at, own] * back
        r.curved[at, own] = curved
        tangent = r.tangent[at, own].astype(F32)
        r.gate_base[at, own] = r.derivative[at, own] * crossing + curved * tangent
        return 0

    def over_error_rows(i, kept):
        at = chunk(i)
        crossing = contract_last(r.outer_low[at, :], r.ee[pl.ds(0, count), :])
        tangent, curved = r.tangent[at, :].astype(F32), r.curved[at, :]
        value = r.derivative[at, :] * crossing + curved * tangent
        r.gate_base[at, over] = value[:, over]
        term = 2.0 * r.both[at, :count].astype(F32) * crossing + curved * tangent * tangent
        return kept + folded(term)

    def gate_pair(q, p):
        at = span(2 * p * wide, 2 * wide, 16)
        w = p + pairs * q
        if q == 0:
            back = contract_last(r.low_down[at, :], r.ee[pl.ds(half, count), :])
            back = pltpu.roll(back, half, 1)
            r.curved[at, over] = r.second[at, over] * back[:, over]
            value = r.gate_base[at, own] + r.derivative[at, own] * back[:, own]
            packed = jnp.concatenate([value[:wide], value[wide:]], axis=1)
        else:
            back = contract_last(r.low_down[at, :], r.ee[pl.ds(count, count), :])
            value = r.gate_base[at, :] + r.derivative[at, :] * back
            packed = pack(1, value[:wide], value[wide:])
        r.part[2, chunk(w), :] = packed.astype(BF)
        first_hop(2, w).start()

    def gate_rows(q):
        at_q = lanes[q]

        def use(w, offset, size):
            ats = []
            for at, part in unpacked(2, q, pairs * q, w, offset, size):
                r.gate[at, at_q] = part[:, at_q].astype(BF)
                ats.append(at)
            if q == 0:
                return
            lowered = product(both_rows(r.gate, ats), r.gram_parts[...])
            lowered = lowered[:, :count] + lowered[:, count:]
            carried = (both_rows(r.derivative, ats) * lowered).astype(BF)
            r.acc[2] += contract_first(carried, both_rows(r.low_down, ats))
            for k, at in enumerate(ats):
                r.carried[at, :] = carried[k * size : (k + 1) * size]
            r.kept[...] += folded(both_rows(r.curved, ats) * lowered * lowered)

        return use

    r.kept[...] = jnp.zeros(r.kept.shape, F32)
    r.gate_gram[...] = jnp.zeros(r.gate_gram.shape, F32)
    r.carry_gram[...] = jnp.zeros(r.carry_gram.shape, F32)
    lax.fori_loop(0, STEPS, own_error_rows, 0)
    forward(2, r.ee, count, t_copies)
    arrived(1)
    for p in range(pairs):
        gate_pair(0, p)
        if p:
            pair_sum(2, p - 1)
    kept = jnp.zeros((8, count), F32)
    for p in range(pairs):
        kept = over_error_rows(2 * p, kept)
        pair_sum(2, pairs + p - 1)
        kept = over_error_rows(2 * p + 1, kept)
        if p == 0:
            arrived(2)
        gate_pair(1, p)
    first_part = summed(kept)
    head, tail = pl.ds(0, count), pl.ds(count, count)
    r.acc[2] = product(r.both_gram[tail, :].astype(BF), r.ee[...])
    gram = contract_last(r.ee[...], r.ee[...])
    h_t = summed(r.both_gram[tail, head] * gram[count:, :count])
    change = 2.0 * h_t + summed(r.both_gram[head, head] * gram[:count, :count])
    change = change + summed(r.both_gram[tail, tail] * gram[count:, count:])
    r.error_gram[...] = gram[:count, :]
    pair_sum(2, STEPS - 1)
    take_chunks(2, gate_rows(0), 0, pairs)
    take_chunks(2, gate_rows(1), pairs, STEPS, prompt=True)
    reduce_start(2)

    def late_rows(i, _):
        at = chunk(i)
        gate = r.gate[at, :]
        r.gate_gram[...] += contract_first(gate, gate)
        r.carry_gram[...] += contract_first(r.carried[at, :], r.both[at, :])
        return 0

    lax.fori_loop(0, STEPS, late_rows, 0)
    change = change + summed(r.gate_gram[...] * r.token_gram[...])
    carry = summed(r.carry_gram[...] * r.error_gram[...])
    final = summed(r.kept[...]) + 2.0 * carry
    reduce_middle(2)

    value = reduce_end(2)
    final = final + summed(weight * (value * value))
    index = lax.broadcasted_iota(jnp.int32, (1, 128), 1)
    value = jnp.zeros((1, 128), F32)
    for at, number in enumerate((norm, first + first_part, change, final)):
        value = value + jnp.where(index == at, number, 0.0)
    r.own[...] = value
    number_copies = [
        remote(r.own, r.slots.at[k], r.all_s, r.all_r, all_places[k])
        for k in range(n * m - 1)
    ]
    for copy in number_copies:
        copy.start()
    drain(r.slots, r.all_r)
    for k in range(n * m - 1):
        value = value + r.slots[k]
    norm, first, change, final = (summed(jnp.where(index == at, value, 0.0)) for at in range(4))
    step = norm / (norm + first)
    keep = first / (norm + first)
    norm_next = keep * keep * norm - 2.0 * keep * step * first + step * step * change
    ratio = norm_next / norm
    curvature = (
        norm_next
        + keep * keep * first
        - 2.0 * keep * step * change
        + step * step * final
        - ratio * norm_next / step
    )
    step_next = norm_next / curvature
    r.sums[0:1, :] = jnp.broadcast_to(step + step_next * (ratio + keep), (1, 128))
    r.sums[1:2, :] = jnp.broadcast_to(-step_next * step, (1, 128))

    for hop in range(bits + 1):
        drain(r.got, r.ex_s.at[hop])
        gram_copy(hop).wait_send()
    for k in range(3):
        drain(r.xx.at[pl.ds(0, (n - 1) * rows), :], r.sp_s.at[k])
        drain(r.half_out.at[k], r.rx_s.at[k])
        drain(r.column_out.at[k], r.rz_s.at[k])
    drain(r.task_slots, r.task_s)
    drain(r.slots, r.all_s)


def fused(n, m, tokens, targets, task, up, outer_up, down, outer_down):
    hid, width = up.shape
    rows = tokens.shape[0]
    count, half, nz = n * rows, n * rows // 2, n // 2
    bits = m.bit_length() - 1
    hp = -(-hid // (2 * 16 * STEPS)) * 16 * STEPS
    total = 2 * hp
    vm, dma = pltpu.VMEM, pltpu.SemaphoreType.DMA
    links = max(bits - 1, 1)
    outs = {
        "gate": ((total, count), BF),
        "both": ((total, 2 * count), BF),
        "xx": ((count, width), BF),
        "ee": ((2 * count, width), BF),
        "ups": ((STEPS, 2, total // STEPS, width), BF),
        "outer_low": ((total, width), BF),
        "sums": ((8, 128), F32),
    }
    scratch = {
        "low_down": vm((total, width), BF),
        "part": vm((3, total, count), BF),
        "got": vm((3, hp, count), BF),
        "sent": vm((3, links, hp, count), BF),
        "wire": vm((3, links, hp, count), BF),
        "full": vm((3, total, count), BF),
        "tangent": vm((total, count), BF),
        "derivative": vm((total, count), F32),
        "second": vm((total, count), F32),
        "curved": vm((total, count), F32),
        "gate_base": vm((total, count), F32),
        "acc": vm((3, count, width), F32),
        "half_out": vm((3, half, width), BF),
        "half_in": vm((3, nz, rows, width), BF),
        "column_out": vm((3, nz - 1, rows, width), BF),
        "column_in": vm((3, nz - 1, rows, width), BF),
        "fresh": vm((2, rows, width), BF),
        "token_gram": vm((count, count), F32),
        "gram_got": vm((half, count), F32),
        "gram_sent": vm((links, half, count), F32),
        "gram_wire": vm((links, half, count), F32),
        "gram_full": vm((count, count), F32),
        "gram_parts": vm((count, 2 * count), BF),
        "both_gram": vm((2 * count, 2 * count), F32),
        "gate_gram": vm((count, count), F32),
        "carry_gram": vm((count, 2 * count), F32),
        "error_gram": vm((count, 2 * count), F32),
        "carried": vm((total, count), BF),
        "kept": vm((8, count), F32),
        "tokens": vm(tokens.shape, BF),
        "targets": vm(targets.shape, BF),
        "task": pltpu.SMEM(task.shape, task.dtype),
        "task_own": vm((8, 128), F32),
        "task_slots": vm((n - 1, 8, 128), F32),
        "own": vm((1, 128), F32),
        "slots": vm((n * m - 1, 1, 128), F32),
        "small_sem": dma((3,)),
        "load_sem": dma((4,)),
        "task_s": dma,
        "task_r": dma,
        "sp_s": dma((3,)),
        "sp_zr": dma((3, nz - 1)),
        "sp_xr": dma((3,)),
        "ex_s": dma((bits + 1,)),
        "ex_r": dma((3, bits + 1, STEPS)),
        "rx_s": dma((3,)),
        "rx_r": dma((3, nz)),
        "rz_s": dma((3,)),
        "rz_r": dma((3,)),
        "gram_s": dma((bits + 1,)),
        "gram_r": dma((bits + 1,)),
        "all_s": dma,
        "all_r": dma,
    }
    inputs = ("task_in", "tokens_in", "targets_in", "up", "outer_up", "down", "outer_down")
    arrays = (task, tokens, targets, up, outer_up, down, outer_down)
    whole = pl.BlockSpec(memory_space=pltpu.VMEM)
    return pl.pallas_call(
        functools.partial(fused_kernel, n, m, hid, inputs + tuple(outs) + tuple(scratch)),
        out_shape=[vm(*o) for o in outs.values()],
        in_specs=[pl.BlockSpec(memory_space=pltpu.HBM)] * len(inputs),
        out_specs=[whole] * len(outs),
        scratch_shapes=list(scratch.values()),
        compiler_params=pltpu.CompilerParams(
            collective_id=0, has_side_effects=True, vmem_limit_bytes=VMEM_LIMIT
        ),
    )(*(pltpu.with_memory_space_constraint(a, pltpu.HBM) for a in arrays))


def output_tiles(hid, wide):
    tiles, start = [], 0
    while start < hid:
        size = 64 if start == 0 else wide // 2
        size = min(size, wide - start % wide, hid - start)
        tiles.append((start, size))
        start += size
    return tiles


def output_kernel(
    gate, both, xx, ee, ups, outer_low, sums, meta_up, meta_down, stage, sems
):
    hid, width = meta_up.shape
    of_outer, of_change = sums[0:1, 0:1], sums[1:2, 0:1]
    wide = ups.shape[2]
    for start, size in output_tiles(hid, wide):
        at, part = pl.ds(start, size), pl.ds(start % wide, size)
        outer = ups[start // wide, 1, part, :].astype(F32)
        stage[0, at, :] = of_outer * outer + of_change * product(gate[at, :], xx[...])
        outer = outer_low[at, :].astype(F32)
        stage[1, at, :] = of_outer * outer + of_change * product(both[at, :], ee[...])
        for k, meta in enumerate((meta_up, meta_down)):
            pltpu.make_async_copy(stage.at[k, at, :], meta.at[at, :], sems.at[k]).start()
    for k, meta in enumerate((meta_up, meta_down)):
        pltpu.make_async_copy(stage.at[k], meta, sems.at[k]).wait()


def outputs(hid, gate, both, xx, ee, ups, outer_low, sums):
    width = xx.shape[1]
    return pl.pallas_call(
        output_kernel,
        out_shape=[jax.ShapeDtypeStruct((hid, width), F32)] * 2,
        in_specs=[pl.BlockSpec(memory_space=pltpu.VMEM)] * 7,
        out_specs=[pl.BlockSpec(memory_space=pltpu.HBM)] * 2,
        scratch_shapes=[
            pltpu.VMEM((2, hid, width), F32),
            pltpu.SemaphoreType.DMA((2,)),
        ],
        compiler_params=pltpu.CompilerParams(vmem_limit_bytes=OUT_LIMIT),
    )(gate, both, xx, ee, ups, outer_low, sums)


def body(n, m, tokens, targets, task_of_token, up_weight, down_weight, outer_up, outer_down):
    results = fused(
        n, m, tokens, targets, task_of_token, up_weight, outer_up, down_weight, outer_down
    )
    return tuple(outputs(up_weight.shape[0], *results))


def solution(mesh):
    placed = tuple(P("dp") if i == 2 else P("dp", "shard") for i in range(7))
    return jax.shard_map(
        functools.partial(body, mesh.shape["dp"], mesh.shape["shard"]),
        mesh=mesh,
        in_specs=placed,
        out_specs=(P("dp", "shard"), P("dp", "shard")),
        check_vma=False,
    )
```

```python
import functools
import types

import jax
import jax.numpy as jnp
from jax import lax
from jax.experimental import pallas as pl
from jax.experimental.pallas import tpu as pltpu
from jax.sharding import PartitionSpec as P

TASKS = 16
STEPS = 4
BF = jnp.bfloat16
F32 = jnp.float32
MESH = pl.DeviceIdType.MESH
VMEM_LIMIT = 44 * 2**20
OUT_LIMIT = 24 * 2**20


def sigmoid_parts(linear_part):
    argument = linear_part.astype(F32)
    logistic = jax.nn.sigmoid(argument)
    derivative = logistic * (1.0 + argument * (1.0 - logistic))
    second_order = logistic * (1.0 - logistic) * (2.0 + argument * (1.0 - 2.0 * logistic))
    return (argument * logistic, derivative, second_order)


def contract_last(left_side, right_side):
    return lax.dot_general(
        left_side, right_side, (((1,), (1,)), ((), ())), preferred_element_type=F32
    )


def contract_first(left_side, right_side):
    return lax.dot_general(
        left_side, right_side, (((0,), (0,)), ((), ())), preferred_element_type=F32
    )


def product(left_side, right_side):
    return jnp.dot(left_side, right_side, preferred_element_type=F32)


def remote(src, dst, send_sem, recv_sem, where):
    return pltpu.make_async_remote_copy(
        src_ref=src,
        dst_ref=dst,
        send_sem=send_sem,
        recv_sem=recv_sem,
        device_id=where,
        device_id_type=MESH,
    )


def summed(term):
    return jnp.sum(jnp.sum(term, axis=1, keepdims=True), axis=0, keepdims=True)


def folded(term):
    return jnp.sum(term.reshape(term.shape[0] // 8, 8, term.shape[1]), axis=0)


def span(start, size, unit):
    return pl.ds(pl.multiple_of(start, unit), size)


def fused_kernel(n, m, hid, names, *refs):
    r = types.SimpleNamespace(**dict(zip(names, refs)))
    rows, width = r.tokens_in.shape
    count, half, nz = n * rows, n * rows // 2, n // 2
    total = r.both.shape[0]
    hp = total // 2
    h = hp // STEPS
    wide = 2 * h
    bits = m.bit_length() - 1
    me = lax.axis_index("dp")
    xx, zz = lax.rem(me, 2), me // 2
    shard = lax.axis_index("shard")
    low = lax.rem(shard, 2)
    partner = {"dp": 2 * zz + 1 - xx}

    def drain(ref, sem):
        pltpu.make_async_copy(ref, ref, sem).wait()

    def across(j):
        to = zz
        for bit in range(nz.bit_length() - 1):
            if j >> bit & 1:
                step = 1 << bit
                to = to + step - 2 * step * lax.rem(zz // step, 2)
        return to

    column = [{"dp": 2 * across(j) + xx} for j in range(nz)]
    far_first = range(nz - 1, 0, -1)
    dp_places = [{"dp": lax.rem(me + k, n)} for k in range(1, n)]
    shard_places = [{"shard": lax.rem(shard + k, m)} for k in range(1, m)]
    all_places = [
        {"dp": lax.rem(me + a, n), "shard": lax.rem(shard + b, m)}
        for a in range(n)
        for b in range(m)
        if a + b
    ]

    def flip(bit):
        step = 1 << bit
        return {"shard": shard + step - 2 * step * lax.rem(shard // step, 2)}

    barrier = pltpu.get_barrier_semaphore()
    for where in all_places:
        pl.semaphore_signal(barrier, inc=1, device_id=where, device_id_type=MESH)
    small = [
        pltpu.make_async_copy(src, dst, r.small_sem.at[i])
        for i, (src, dst) in enumerate(
            ((r.task_in, r.task), (r.tokens_in, r.tokens), (r.targets_in, r.targets))
        )
    ]
    small[1].start()
    small[0].start()

    def load(src, dst, step, index):
        size = min(wide, hid - step * wide)
        return pltpu.make_async_copy(
            src.at[pl.ds(step * wide, size)], dst.at[pl.ds(0, size)], r.load_sem.at[index]
        )

    loads = []
    for step in range(STEPS):
        if step * wide < hid:
            loads.append(load(r.up, r.ups.at[step, 0], step, 0))
            loads.append(load(r.outer_up, r.ups.at[step, 1], step, 1))
    for step in range(STEPS):
        if step * wide < hid:
            loads.append(load(r.down, r.low_down.at[pl.ds(step * wide, wide)], step, 2))
            loads.append(load(r.outer_down, r.outer_low.at[pl.ds(step * wide, wide)], step, 3))
    small[1].wait()
    small[0].wait()
    for copy in loads + small[2:]:
        copy.start()

    block = span(zz * rows, rows, rows)
    r.xx[block, :] = r.tokens[...]
    for step in range(STEPS):
        gap = min(wide, (step + 1) * wide - hid)
        if gap > 0:
            r.ups[step, :, pl.ds(wide - gap, gap), :] = jnp.zeros((2, gap, width), BF)
    if total > hid:
        r.low_down[pl.ds(hid, total - hid), :] = jnp.zeros((total - hid, width), BF)
        r.outer_low[pl.ds(hid, total - hid), :] = jnp.zeros((total - hid, width), BF)
    r.acc[...] = jnp.zeros(r.acc.shape, F32)

    pl.semaphore_wait(barrier, n * m - 1)

    def spread(s, src, dst, offset):
        near = span(offset + zz * rows, rows, rows)
        over = span(offset + half + zz * rows, rows, rows)
        out = [
            remote(src, dst.at[near, :], r.sp_s.at[s], r.sp_zr.at[s, j - 1], column[j])
            for j in far_first
        ]
        out.append(remote(src, dst.at[over, :], r.sp_s.at[s], r.sp_xr.at[s], partner))
        for copy in out:
            copy.start()
        return out

    def forward(s, dst, offset, out):
        for j in range(1, nz):
            out[nz - 1 - j].wait_recv()
            at = span(offset + across(j) * rows, rows, rows)
            over = span(offset + half + across(j) * rows, rows, rows)
            copy = remote(
                dst.at[at, :], dst.at[over, :], r.sp_s.at[s], r.sp_xr.at[s], partner
            )
            copy.start()

    def arrived(s):
        drain(r.xx.at[pl.ds(0, half), :], r.sp_xr.at[s])

    token_copies = spread(0, r.tokens, r.xx, 0)

    lane = lax.broadcasted_iota(jnp.int32, (8, 128), 1)
    line = lax.broadcasted_iota(jnp.int32, (rows, 128), 0)
    own_row = jnp.full((8, 128), -1.0, F32)
    own_col = jnp.zeros((rows, 128), F32)
    for i in range(rows):
        number = r.task[i].astype(F32)
        own_row = jnp.where(lane == i, number, own_row)
        own_col = jnp.where(line == i, number, own_col)
    r.task_own[...] = own_row
    task_copies = [
        remote(r.task_own, r.task_slots.at[k], r.task_s, r.task_r, dp_places[k])
        for k in range(n - 1)
    ]
    for copy in task_copies:
        copy.start()
    forward(0, r.xx, 0, token_copies)
    arrived(0)
    small[2].wait()
    for i in range(4):
        drain(r.low_down.at[pl.ds(0, hid), :], r.load_sem.at[i])
    tokens = r.xx

    def chunk(i):
        return span(i * wide, wide, 16)

    def own_part(i):
        return span(i * wide + low * h, h, 16)

    def strip(i):
        return span(i * h, h, 16)

    full = [r.full.at[0], r.full.at[1], r.full.at[2]]
    pairs = STEPS // 2
    lanes = [slice(0, half), slice(half, count)]

    def side(shape):
        return lax.broadcasted_iota(jnp.int32, shape, 1) < half

    def pack(q, top, bottom):
        if q == 0:
            return jnp.where(side(top.shape), top, pltpu.roll(bottom, half, 1))
        return jnp.where(side(top.shape), pltpu.roll(top, half, 1), bottom)

    def unpack(q, packed):
        turned = pltpu.roll(packed, half, 1)
        return (packed, turned) if q == 0 else (turned, packed)

    def first_hop(s, i):
        away = span(i * wide + (1 - low) * h, h, 16)
        return remote(
            r.part.at[s, away, :], r.got.at[s, strip(i), :], r.ex_s.at[0], r.ex_r.at[s, 0, i], flip(0)
        )

    def wire_hop(s, bit, i):
        return remote(
            r.sent.at[s, bit - 1, strip(i), :],
            r.wire.at[s, bit - 1, strip(i), :],
            r.ex_s.at[bit],
            r.ex_r.at[s, bit, i],
            flip(bit),
        )

    def last_hop(s, i):
        at = own_part(i)
        return remote(
            full[s].at[at, :], full[s].at[at, :], r.ex_s.at[bits], r.ex_r.at[s, bits, i], flip(0)
        )

    def pair_sum(s, i):
        first_hop(s, i).wait_recv()
        value = r.part[s, own_part(i), :].astype(F32) + r.got[s, strip(i), :].astype(F32)
        r.sent[s, 0, strip(i), :] = value.astype(BF)
        wire_hop(s, 1, i).start()

    def take_chunks(s, use, begin, end, prompt=False):
        def step(i, _):
            for bit in range(1, bits):
                wire_hop(s, bit, i).wait_recv()
                value = r.sent[s, bit - 1, strip(i), :].astype(F32)
                value = (value + r.wire[s, bit - 1, strip(i), :].astype(F32)).astype(BF)
                if bit + 1 < bits:
                    r.sent[s, bit, strip(i), :] = value
                    wire_hop(s, bit + 1, i).start()
            full[s][own_part(i), :] = value
            last_hop(s, i).start()
            if prompt:
                use(i, low * h, h)
                last_hop(s, i).wait_recv()
                use(i, (1 - low) * h, h)
                return 0

            @pl.when(i > begin)
            def _():
                last_hop(s, i - 1).wait_recv()
                use(i - 1, (1 - low) * h, h)

            use(i, low * h, h)
            return 0

        lax.fori_loop(begin, end, step, 0)
        if not prompt:
            last_hop(s, end - 1).wait_recv()
            use(end - 1, (1 - low) * h, h)

    def linear_step(p, _):
        parts = []
        for e in range(2):
            i = 2 * p + e
            value = contract_last(r.ups[i].reshape(2 * wide, width), tokens[...])
            r.part[0, chunk(i), :] = value[:wide].astype(BF)
            parts.append(value[wide:])
            first_hop(0, i).start()
            if e:
                pair_sum(0, i - 1)
            else:

                @pl.when(p > 0)
                def _():
                    pair_sum(0, i - 1)

        for q in (1, 0):
            w = p + pairs * (1 - q)
            r.part[1, chunk(w), :] = pack(q, *parts).astype(BF)
            first_hop(1, w).start()
        return 0

    def hidden_rows(i, offset, size):
        at = span(i * wide + offset, size, 16)
        activation, derivative, second_order = sigmoid_parts(r.full[0, at, :])
        hidden = activation.astype(BF)
        r.both[at, count:] = hidden
        r.derivative[at, :] = derivative
        r.second[at, :] = second_order
        r.acc[0] += contract_first(hidden, r.low_down[at, :])
        r.acc[1] += contract_first(hidden, r.outer_low[at, :])

    def unpacked(s, q, first, w, offset, size):
        packed = full[s][span(w * wide + offset, size, 16), :].astype(F32)
        p = w - first
        return [
            (span((2 * p + e) * wide + offset, size, 16), part)
            for e, part in enumerate(unpack(q, packed))
        ]

    def both_rows(ref, ats):
        return jnp.concatenate([ref[at, :] for at in ats], axis=0)

    def tangent_rows(q):
        at_q = lanes[q]

        def use(w, offset, size):
            ats, changes = [], []
            for at, tangent in unpacked(1, q, pairs * (1 - q), w, offset, size):
                change = (r.derivative[at, :] * tangent).astype(BF)
                r.both[at, at_q] = change[:, at_q]
                r.tangent[at, at_q] = tangent[:, at_q].astype(BF)
                ats.append(at)
                changes.append(change)
            change = jnp.concatenate(changes, axis=0)
            r.acc[1, at_q] += contract_first(change, both_rows(r.low_down, ats))[at_q]

        return use

    def half_place(j):
        return span(across(j) * rows, rows, rows)

    def half_copy(s, j):
        return remote(
            r.half_out.at[s, half_place(j), :], r.half_in.at[s, j], r.rx_s.at[s], r.rx_r.at[s, j], partner
        )

    def column_copy(s, j):
        return remote(
            r.column_out.at[s, j - 1], r.column_in.at[s, j - 1], r.rz_s.at[s], r.rz_r.at[s], column[j]
        )

    def reduce_start(s):
        r.half_out[s] = r.acc[s, pl.ds(half, half), :].astype(BF)
        for j in range(nz - 1, -1, -1):
            half_copy(s, j).start()

    def pair_rows(s, j):
        half_copy(s, j).wait_recv()
        return r.acc[s, half_place(j), :] + r.half_in[s, j].astype(F32)

    def reduce_middle(s):
        for j in far_first:
            r.column_out[s, j - 1] = pair_rows(s, j).astype(BF)
            column_copy(s, j).start()

    def reduce_end(s):
        value = pair_rows(s, 0)
        drain(r.column_in.at[s], r.rz_r.at[s])
        for j in range(1, nz):
            value = value + r.column_in[s, j - 1].astype(F32)
        return value

    k_mine, k_other = span(low * half, half, half), span((1 - low) * half, half, half)

    def gram_copy(j):
        if j == 0:
            src, dst = r.token_gram.at[k_other, :], r.gram_got
        elif j < bits:
            src, dst = r.gram_sent.at[j - 1], r.gram_wire.at[j - 1]
        else:
            src, dst = r.gram_full.at[k_mine, :], r.gram_full.at[k_mine, :]
        return remote(src, dst, r.gram_s.at[j], r.gram_r.at[j], flip(0 if j == bits else j))

    def gram_step(j):
        if j == 0:
            r.token_gram[...] = contract_last(tokens[...], tokens[...])
            gram_copy(0).start()
            return
        gram_copy(j - 1).wait_recv()
        if j == 1:
            value = r.token_gram[k_mine, :] + r.gram_got[...]
        elif j <= bits:
            value = r.gram_sent[j - 2] + r.gram_wire[j - 2]
        if j < bits:
            r.gram_sent[j - 1] = value
        elif j == bits:
            r.gram_full[k_mine, :] = value
        if j <= bits:
            gram_copy(j).start()
            return
        high = r.gram_full[...].astype(BF)
        r.gram_parts[:, :count] = high
        r.gram_parts[:, count:] = (r.gram_full[...] - high.astype(F32)).astype(BF)

    lax.fori_loop(0, pairs, linear_step, 0)
    pair_sum(0, STEPS - 1)
    lax.fori_loop(0, STEPS, lambda i, _: (pair_sum(1, i), 0)[1], 0)
    gram_step(0)
    take_chunks(0, hidden_rows, 0, STEPS)
    reduce_start(0)
    gram_step(1)
    take_chunks(1, tangent_rows(1), 0, pairs)
    reduce_start(1)
    reduce_middle(0)
    take_chunks(1, tangent_rows(0), pairs, STEPS)
    reduce_middle(1)
    for j in range(2, bits + 1):
        gram_step(j)

    same = jnp.where(own_row[0:1, :] == own_col, 1.0, 0.0)
    drain(r.task_slots, r.task_r)
    for k in range(n - 1):
        same = same + jnp.where(r.task_slots[k, 0:1, :] == own_col, 1.0, 0.0)
    weight = 1.0 / (TASKS * jnp.sum(same, axis=1, keepdims=True))

    value = reduce_end(0)
    r.fresh[0] = (weight * (value - r.targets[...].astype(F32))).astype(BF)
    r.ee[block, :] = r.fresh[0]
    e_copies = spread(1, r.fresh.at[0], r.ee, 0)

    def gram_rows(i, _):
        at = chunk(i)
        r.both_gram[...] += contract_first(r.both[at, :], r.both[at, :])
        return 0

    r.both_gram[...] = jnp.zeros(r.both_gram.shape, F32)
    lax.fori_loop(0, STEPS, gram_rows, 0)

    def low_squares(i, kept):
        for step in range(STEPS):
            one = r.outer_low[span(step * wide + i * 16, 16, 16), :].astype(F32)
            kept = kept + one * one
        return kept

    def up_squares(i, kept):
        for step in range(STEPS):
            one = r.ups[step, 1, span(i * 16, 16, 16), :].astype(F32)
            kept = kept + one * one
        return kept

    norm = summed(lax.fori_loop(0, wide // 16, low_squares, jnp.zeros((16, width), F32)))
    gram_step(bits + 1)
    value = reduce_end(1)
    first = summed(weight * (value * value))
    r.fresh[1] = (weight * value).astype(BF)
    r.ee[span(count + zz * rows, rows, rows), :] = r.fresh[1]
    t_copies = spread(2, r.fresh.at[1], r.ee, count)
    forward(1, r.ee, 0, e_copies)

    own, over = lanes

    def own_error_rows(i, _):
        at = chunk(i)
        errors = r.ee[pl.ds(0, half), :]
        back = contract_last(r.low_down[at, :], errors)
        crossing = contract_last(r.outer_low[at, :], errors)
        curved = r.second[at, own] * back
        r.curved[at, own] = curved
        tangent = r.tangent[at, own].astype(F32)
        r.gate_base[at, own] = r.derivative[at, own] * crossing + curved * tangent
        return 0

    def over_error_rows(i, kept):
        at = chunk(i)
        crossing = contract_last(r.outer_low[at, :], r.ee[pl.ds(0, count), :])
        tangent, curved = r.tangent[at, :].astype(F32), r.curved[at, :]
        value = r.derivative[at, :] * crossing + curved * tangent
        r.gate_base[at, over] = value[:, over]
        term = 2.0 * r.both[at, :count].astype(F32) * crossing + curved * tangent * tangent
        return kept + folded(term)

    def gate_pair(q, p):
        at = span(2 * p * wide, 2 * wide, 16)
        w = p + pairs * q
        if q == 0:
            back = contract_last(r.low_down[at, :], r.ee[pl.ds(half, count), :])
            back = pltpu.roll(back, half, 1)
            r.curved[at, over] = r.second[at, over] * back[:, over]
            value = r.gate_base[at, own] + r.derivative[at, own] * back[:, own]
            packed = jnp.concatenate([value[:wide], value[wide:]], axis=1)
        else:
            back = contract_last(r.low_down[at, :], r.ee[pl.ds(count, count), :])
            value = r.gate_base[at, :] + r.derivative[at, :] * back
            packed = pack(1, value[:wide], value[wide:])
        r.part[2, chunk(w), :] = packed.astype(BF)
        first_hop(2, w).start()

    def gate_rows(q):
        at_q = lanes[q]

        def use(w, offset, size):
            ats = []
            for at, part in unpacked(2, q, pairs * q, w, offset, size):
                r.gate[at, at_q] = part[:, at_q].astype(BF)
                ats.append(at)
            if q == 0:
                return
            lowered = product(both_rows(r.gate, ats), r.gram_parts[...])
            lowered = lowered[:, :count] + lowered[:, count:]
            carried = (both_rows(r.derivative, ats) * lowered).astype(BF)
            r.acc[2] += contract_first(carried, both_rows(r.low_down, ats))
            for k, at in enumerate(ats):
                r.carried[at, :] = carried[k * size : (k + 1) * size]
            r.kept[...] += folded(both_rows(r.curved, ats) * lowered * lowered)

        return use

    r.kept[...] = jnp.zeros(r.kept.shape, F32)
    r.gate_gram[...] = jnp.zeros(r.gate_gram.shape, F32)
    r.carry_gram[...] = jnp.zeros(r.carry_gram.shape, F32)
    lax.fori_loop(0, STEPS, own_error_rows, 0)
    forward(2, r.ee, count, t_copies)
    arrived(1)
    for p in range(pairs):
        gate_pair(0, p)
        if p:
            pair_sum(2, p - 1)
    kept = jnp.zeros((8, count), F32)
    for p in range(pairs):
        kept = over_error_rows(2 * p, kept)
        pair_sum(2, pairs + p - 1)
        kept = over_error_rows(2 * p + 1, kept)
        if p == 0:
            arrived(2)
        gate_pair(1, p)
    first_part = summed(kept)
    head, tail = pl.ds(0, count), pl.ds(count, count)
    r.acc[2] = product(r.both_gram[tail, :].astype(BF), r.ee[...])
    gram = contract_last(r.ee[...], r.ee[...])
    h_t = summed(r.both_gram[tail, head] * gram[count:, :count])
    change = 2.0 * h_t + summed(r.both_gram[head, head] * gram[:count, :count])
    change = change + summed(r.both_gram[tail, tail] * gram[count:, count:])
    r.error_gram[...] = gram[:count, :]
    pair_sum(2, STEPS - 1)
    take_chunks(2, gate_rows(0), 0, pairs)
    take_chunks(2, gate_rows(1), pairs, STEPS, prompt=True)
    reduce_start(2)

    def late_rows(i, _):
        at = chunk(i)
        gate = r.gate[at, :]
        r.gate_gram[...] += contract_first(gate, gate)
        r.carry_gram[...] += contract_first(r.carried[at, :], r.both[at, :])
        return 0

    lax.fori_loop(0, STEPS, late_rows, 0)
    change = change + summed(r.gate_gram[...] * r.token_gram[...])
    carry = summed(r.carry_gram[...] * r.error_gram[...])
    final = summed(r.kept[...]) + 2.0 * carry
    reduce_middle(2)
    norm = norm + summed(lax.fori_loop(0, wide // 16, up_squares, jnp.zeros((16, width), F32)))

    value = reduce_end(2)
    final = final + summed(weight * (value * value))
    index = lax.broadcasted_iota(jnp.int32, (1, 128), 1)
    value = jnp.zeros((1, 128), F32)
    for at, number in enumerate((norm, first + first_part, change, final)):
        value = value + jnp.where(index == at, number, 0.0)
    r.own[...] = value
    number_copies = [
        remote(r.own, r.slots.at[k], r.all_s, r.all_r, all_places[k])
        for k in range(n * m - 1)
    ]
    for copy in number_copies:
        copy.start()
    drain(r.slots, r.all_r)
    for k in range(n * m - 1):
        value = value + r.slots[k]
    norm, first, change, final = (summed(jnp.where(index == at, value, 0.0)) for at in range(4))
    step = norm / (norm + first)
    keep = first / (norm + first)
    norm_next = keep * keep * norm - 2.0 * keep * step * first + step * step * change
    ratio = norm_next / norm
    curvature = (
        norm_next
        + keep * keep * first
        - 2.0 * keep * step * change
        + step * step * final
        - ratio * norm_next / step
    )
    step_next = norm_next / curvature
    r.sums[0:1, :] = jnp.broadcast_to(step + step_next * (ratio + keep), (1, 128))
    r.sums[1:2, :] = jnp.broadcast_to(-step_next * step, (1, 128))

    for hop in range(bits + 1):
        drain(r.got, r.ex_s.at[hop])
        gram_copy(hop).wait_send()
    for k in range(3):
        drain(r.xx.at[pl.ds(0, (n - 1) * rows), :], r.sp_s.at[k])
        drain(r.half_out.at[k], r.rx_s.at[k])
        drain(r.column_out.at[k], r.rz_s.at[k])
    drain(r.task_slots, r.task_s)
    drain(r.slots, r.all_s)


def fused(n, m, tokens, targets, task, up, outer_up, down, outer_down):
    hid, width = up.shape
    rows = tokens.shape[0]
    count, half, nz = n * rows, n * rows // 2, n // 2
    bits = m.bit_length() - 1
    hp = -(-hid // (2 * 16 * STEPS)) * 16 * STEPS
    total = 2 * hp
    vm, dma = pltpu.VMEM, pltpu.SemaphoreType.DMA
    links = max(bits - 1, 1)
    outs = {
        "gate": ((total, count), BF),
        "both": ((total, 2 * count), BF),
        "xx": ((count, width), BF),
        "ee": ((2 * count, width), BF),
        "ups": ((STEPS, 2, total // STEPS, width), BF),
        "outer_low": ((total, width), BF),
        "sums": ((8, 128), F32),
    }
    scratch = {
        "low_down": vm((total, width), BF),
        "part": vm((3, total, count), BF),
        "got": vm((3, hp, count), BF),
        "sent": vm((3, links, hp, count), BF),
        "wire": vm((3, links, hp, count), BF),
        "full": vm((3, total, count), BF),
        "tangent": vm((total, count), BF),
        "derivative": vm((total, count), F32),
        "second": vm((total, count), F32),
        "curved": vm((total, count), F32),
        "gate_base": vm((total, count), F32),
        "acc": vm((3, count, width), F32),
        "half_out": vm((3, half, width), BF),
        "half_in": vm((3, nz, rows, width), BF),
        "column_out": vm((3, nz - 1, rows, width), BF),
        "column_in": vm((3, nz - 1, rows, width), BF),
        "fresh": vm((2, rows, width), BF),
        "token_gram": vm((count, count), F32),
        "gram_got": vm((half, count), F32),
        "gram_sent": vm((links, half, count), F32),
        "gram_wire": vm((links, half, count), F32),
        "gram_full": vm((count, count), F32),
        "gram_parts": vm((count, 2 * count), BF),
        "both_gram": vm((2 * count, 2 * count), F32),
        "gate_gram": vm((count, count), F32),
        "carry_gram": vm((count, 2 * count), F32),
        "error_gram": vm((count, 2 * count), F32),
        "carried": vm((total, count), BF),
        "kept": vm((8, count), F32),
        "tokens": vm(tokens.shape, BF),
        "targets": vm(targets.shape, BF),
        "task": pltpu.SMEM(task.shape, task.dtype),
        "task_own": vm((8, 128), F32),
        "task_slots": vm((n - 1, 8, 128), F32),
        "own": vm((1, 128), F32),
        "slots": vm((n * m - 1, 1, 128), F32),
        "small_sem": dma((3,)),
        "load_sem": dma((4,)),
        "task_s": dma,
        "task_r": dma,
        "sp_s": dma((3,)),
        "sp_zr": dma((3, nz - 1)),
        "sp_xr": dma((3,)),
        "ex_s": dma((bits + 1,)),
        "ex_r": dma((3, bits + 1, STEPS)),
        "rx_s": dma((3,)),
        "rx_r": dma((3, nz)),
        "rz_s": dma((3,)),
        "rz_r": dma((3,)),
        "gram_s": dma((bits + 1,)),
        "gram_r": dma((bits + 1,)),
        "all_s": dma,
        "all_r": dma,
    }
    inputs = ("task_in", "tokens_in", "targets_in", "up", "outer_up", "down", "outer_down")
    arrays = (task, tokens, targets, up, outer_up, down, outer_down)
    whole = pl.BlockSpec(memory_space=pltpu.VMEM)
    return pl.pallas_call(
        functools.partial(fused_kernel, n, m, hid, inputs + tuple(outs) + tuple(scratch)),
        out_shape=[vm(*o) for o in outs.values()],
        in_specs=[pl.BlockSpec(memory_space=pltpu.HBM)] * len(inputs),
        out_specs=[whole] * len(outs),
        scratch_shapes=list(scratch.values()),
        compiler_params=pltpu.CompilerParams(
            collective_id=0, has_side_effects=True, vmem_limit_bytes=VMEM_LIMIT
        ),
    )(*(pltpu.with_memory_space_constraint(a, pltpu.HBM) for a in arrays))


def output_tiles(hid, wide):
    tiles, start = [], 0
    while start < hid:
        size = 64 if start == 0 else wide // 2
        size = min(size, wide - start % wide, hid - start)
        tiles.append((start, size))
        start += size
    return tiles


def output_kernel(
    gate, both, xx, ee, ups, outer_low, sums, meta_up, meta_down, stage, sems
):
    hid, width = meta_up.shape
    of_outer, of_change = sums[0:1, 0:1], sums[1:2, 0:1]
    wide = ups.shape[2]
    for start, size in output_tiles(hid, wide):
        at, part = pl.ds(start, size), pl.ds(start % wide, size)
        outer = ups[start // wide, 1, part, :].astype(F32)
        stage[0, at, :] = of_outer * outer + of_change * product(gate[at, :], xx[...])
        outer = outer_low[at, :].astype(F32)
        stage[1, at, :] = of_outer * outer + of_change * product(both[at, :], ee[...])
        for k, meta in enumerate((meta_up, meta_down)):
            pltpu.make_async_copy(stage.at[k, at, :], meta.at[at, :], sems.at[k]).start()
    for k, meta in enumerate((meta_up, meta_down)):
        pltpu.make_async_copy(stage.at[k], meta, sems.at[k]).wait()


def outputs(hid, gate, both, xx, ee, ups, outer_low, sums):
    width = xx.shape[1]
    return pl.pallas_call(
        output_kernel,
        out_shape=[jax.ShapeDtypeStruct((hid, width), F32)] * 2,
        in_specs=[pl.BlockSpec(memory_space=pltpu.VMEM)] * 7,
        out_specs=[pl.BlockSpec(memory_space=pltpu.HBM)] * 2,
        scratch_shapes=[
            pltpu.VMEM((2, hid, width), F32),
            pltpu.SemaphoreType.DMA((2,)),
        ],
        compiler_params=pltpu.CompilerParams(vmem_limit_bytes=OUT_LIMIT),
    )(gate, both, xx, ee, ups, outer_low, sums)


def body(n, m, tokens, targets, task_of_token, up_weight, down_weight, outer_up, outer_down):
    results = fused(
        n, m, tokens, targets, task_of_token, up_weight, outer_up, down_weight, outer_down
    )
    return tuple(outputs(up_weight.shape[0], *results))


def solution(mesh):
    placed = tuple(P("dp") if i == 2 else P("dp", "shard") for i in range(7))
    return jax.shard_map(
        functools.partial(body, mesh.shape["dp"], mesh.shape["shard"]),
        mesh=mesh,
        in_specs=placed,
        out_specs=(P("dp", "shard"), P("dp", "shard")),
        check_vma=False,
    )
```
